128 devices in a mesh: row: 16 (over y, x), col: 8 (over z, core).
Axes of the slice: x: 4, y: 4, z: 4, core: 2. Of those that a mesh axis runs over, the one named last changes fastest.
Arguments:
- trailing: float32 [16384, 16384], P('row', 'col'), may hold values from -36 to 36
- reflectors: float32 [4, 16384, 64], P(None, 'row'), may hold values from -0.046875 to 0.046875
Outputs:
- rotated: float32 [16384, 16384], P('row', 'col')
The draws below stay inside these ranges and needn't reach their ends.
All inputs are finite; a program needn't handle non-finite values.
Results may differ from the reference program's by a relative error of at most 0.00015.
Values sent between devices are 32-bit elements; how exact they have to be, the bound alone decides.
A program may use at most 128 MiB of HBM per device.

```python
import jax
import jax.numpy as jnp
from jax import lax

ORDER = 16384
NB = 64
PANELS = 4


def draw_trailing(key, part):
    base = jnp.clip(jax.random.normal(key, (ORDER, ORDER), jnp.float32), -6.0, 6.0)
    symmetric = (base + base.T) * 0.7071
    return symmetric.astype(jnp.float32)


def shard_levels(rng, shape, pieces, low, high):
    gain = 1.0
    for axis_at, blocks in pieces:
        steps = jax.random.uniform(jax.random.fold_in(jax.random.fold_in(rng, 6), axis_at), (blocks,), jnp.float32, low / len(pieces), high / len(pieces))
        gain = gain * jnp.repeat(jnp.exp(steps), shape[axis_at] // blocks).reshape((-1,) + (1,) * (len(shape) - 1 - axis_at))
    return gain


def centred(stream_key, shape, deviation, most, pieces=(), kind=jnp.bfloat16):
    values = deviation * jax.random.normal(stream_key, shape, jnp.float32)
    if pieces:
        values = values * shard_levels(stream_key, shape, pieces, -0.22, 0.18)
    return jnp.clip(values, -most, most).astype(kind)


def setup_inputs(seed: int = 0) -> dict:
    keys = jax.random.split(jax.random.key(seed), 3)
    trailing = draw_trailing(jax.random.fold_in(keys[2], 71), 0)
    reflectors = centred(keys[1], (PANELS, ORDER, NB), ORDER ** -0.5, 0.046875, ((1, 16),), jnp.float32)
    return dict(trailing=trailing, reflectors=reflectors)


def product(left, right):
    return jnp.dot(left, right, precision=lax.Precision.HIGHEST, preferred_element_type=jnp.float32)


def unit_lower(raw_panels, first_row):
    shape = raw_panels.shape
    widths = shape[2]
    global_row = first_row + lax.broadcasted_iota(jnp.int32, shape, 1)
    pivot_row = (lax.broadcasted_iota(jnp.int32, shape, 0) + 1) * widths + lax.broadcasted_iota(jnp.int32, shape, 2)
    ones_part = jnp.where(global_row == pivot_row, jnp.ones_like(raw_panels), jnp.zeros_like(raw_panels))
    return jnp.where(global_row > pivot_row, raw_panels, ones_part)


def block_factor(gram_block):
    widths = gram_block.shape[0]
    row_ids = lax.broadcasted_iota(jnp.int32, (widths, widths), 0)
    col_ids = lax.broadcasted_iota(jnp.int32, (widths, widths), 1)
    identity = jnp.where(row_ids == col_ids, jnp.ones_like(gram_block), jnp.zeros_like(gram_block))
    halves = jnp.sum(gram_block * identity, axis=0) * 0.5
    strict = jnp.where(col_ids > row_ids, gram_block, jnp.zeros_like(gram_block))
    negated = -(strict / halves[None, :])
    inverse = identity + negated
    power = negated
    reach = 2
    while reach < widths:
        power = product(power, power)
        inverse = product(inverse, identity + power)
        reach = reach * 2
    return inverse / halves[:, None]


def reference(trailing, reflectors):
    panels = unit_lower(reflectors, 0)
    gram_all = jnp.einsum("kin,kim->knm", panels, panels, precision=lax.Precision.HIGHEST)
    matrix = trailing
    for step_index in range(PANELS):
        own_panel = panels[step_index]
        factor = block_factor(gram_all[step_index])
        applied = product(product(matrix, own_panel), factor)
        coupling = product(factor.T, product(own_panel.T, applied))
        update_rows = applied - 0.5 * product(own_panel, coupling)
        left_side = jnp.concatenate([own_panel, update_rows], axis=1)
        right_side = jnp.concatenate([update_rows, own_panel], axis=1)
        matrix = matrix - product(left_side, right_side.T)
    return matrix
```

```python
import functools

import jax
import jax.numpy as jnp
from jax import lax
from jax.experimental import pallas as pl
from jax.experimental.pallas import tpu as pltpu
from jax.sharding import PartitionSpec as P

MESH = pl.DeviceIdType.MESH
F32 = jnp.float32
BF16 = jnp.bfloat16
DELTAS = (0, 1, 3, 2)


def exact(left, right, dims):
    return lax.dot_general(
        left, right, (dims, ((), ())), precision=lax.Precision.HIGHEST, preferred_element_type=F32
    )


def quick(left, right, dims):
    return lax.dot_general(left, right, (dims, ((), ())), preferred_element_type=F32)


def split(value):
    high = value.astype(BF16)
    low = (value - high.astype(F32)).astype(BF16)
    return high, low


NN = ((1,), (0,))
NT = ((1,), (1,))
TN = ((0,), (0,))


def unit_lower(raw_panels, first_row):
    shape = raw_panels.shape
    widths = shape[2]
    global_row = first_row + lax.broadcasted_iota(jnp.int32, shape, 1)
    pivot_row = (lax.broadcasted_iota(jnp.int32, shape, 0) + 1) * widths + lax.broadcasted_iota(
        jnp.int32, shape, 2
    )
    ones_part = jnp.where(
        global_row == pivot_row, jnp.ones_like(raw_panels), jnp.zeros_like(raw_panels)
    )
    return jnp.where(global_row > pivot_row, raw_panels, ones_part)


def exchange_kernel(
    a_hbm, v_ref,
    lhi_ref, llo_ref, rc_hbm,
    a_buf, a_hi, a_lo, vc, yc, yp, drx, yh, zrx, ys, yr,
    pb, xb, yb, gb, pw, inv, mm,
    a_sem, out_sem,
    t_send, t_recv, y_send, y_recv, x_send, x_recv,
    d_send, d_recv, zr_send, zr_recv, za_send, za_recv, e_send, e_recv,
    gx_send, gx_recv, gy_send, gy_recv, gg_send, gg_recv,
):
    row = lax.axis_index("row")
    col = lax.axis_index("col")
    x, y = row % 4, row // 4
    z, k = col // 2, col % 2

    def dev(dx, dy, dz, dk):
        return (dy * 4 + dx, dz * 2 + dk)

    def copy_to(src, dst, send, recv, device):
        return pltpu.make_async_remote_copy(
            src_ref=src, dst_ref=dst, send_sem=send, recv_sem=recv,
            device_id=device, device_id_type=MESH,
        )

    def arrived(dst, recv):
        copy_to(dst, dst, recv, recv, dev(x, y, z, 1 - k)).wait_recv()

    sent = []

    def send(copy, cond=None):
        if cond is None:
            copy.start()
        else:
            pl.when(cond)(copy.start)
        sent.append((copy, cond))

    is_src = k == x // 2
    b_own = x % 2
    stays = jnp.logical_and(y == z, is_src)

    def slab(i):
        return pltpu.make_async_copy(
            a_hbm.at[:, pl.ds(i * 256, 256)], a_buf.at[i], a_sem.at[i]
        )

    for i in range(8):
        slab(i).start()

    barrier = pltpu.get_barrier_semaphore()

    def greet(device):
        pl.semaphore_signal(barrier, inc=1, device_id=device, device_id_type=MESH)

    for d in range(1, 4):
        greet(dev((x + d) % 4, y, z, k))
        greet(dev(x, (y + d) % 4, z, k))
    for d in range(1, 8):
        greet((row, (col + d) % 8))

    @pl.when(y != z)
    def _():
        greet(dev(x, z, y, 0))
        greet(dev(x, z, y, 1))

    pl.semaphore_wait(barrier, jnp.where(y != z, 15, 13))

    def t_start(ph, q):
        target = vc if ph == 0 else yc
        source = v_ref.at[q, z, k] if ph == 0 else ys.at[q]
        place = target.at[q, b_own, z, k]
        send(
            copy_to(source, place, t_send.at[ph, q], t_recv.at[ph, q, k], dev(x, z, y, x // 2)),
            jnp.logical_not(stays),
        )

        @pl.when(stays)
        def _():
            if ph == 0:
                vc[q, b_own, z, k] = v_ref[q, z, k]
            else:
                yc[q, b_own, z, k] = ys[q]

    def y_start(ph, q):
        target = vc if ph == 0 else yc

        @pl.when(is_src)
        def _():
            for h in range(2):
                @pl.when(jnp.logical_not(jnp.logical_and(y == z, k == h)))
                def _():
                    arrived(target.at[q, b_own, y, h], t_recv.at[ph, q, h])

        unit = target.at[q, b_own, y]
        for d in range(1, 4):
            send(
                copy_to(unit, unit, y_send.at[ph, q, d - 1], y_recv.at[ph, q, y],
                        dev(x, (y + d) % 4, z, k)),
                is_src,
            )

    def x_own(ph, q, delta):
        target = vc if ph == 0 else yc
        j = (y + 4 - delta) % 4
        unit = target.at[q, b_own, j]
        if delta:
            @pl.when(is_src)
            def _():
                arrived(unit, y_recv.at[ph, q, j])
        for s, step in enumerate((1, 3)):
            send(
                copy_to(unit, unit, x_send.at[ph, q, 0, delta, s], x_recv.at[ph, q, b_own, j],
                        dev((x + step) % 4, y, z, k)),
                is_src,
            )

    def x_take(ph, q, delta, b):
        target = vc if ph == 0 else yc
        j = (y + 4 - delta) % 4
        far = (x + 4 - (2 * k + b)) % 4
        unit = target.at[q, b, j]

        @pl.when(far != 0)
        def _():
            arrived(unit, x_recv.at[ph, q, b, j])

        onward = 1 if delta in (0, 3) else 3
        send(
            copy_to(unit, unit, x_send.at[ph, q, 1 + b, delta, 0], x_recv.at[ph, q, b, j],
                    dev((x + onward) % 4, y, z, k)),
            far == onward,
        )

    def multiply(q, delta, b):
        j = (y + 4 - delta) % 4
        high, low = split(vc[q, b, j].reshape(256, 128))
        both = jnp.concatenate([high, low], axis=1)
        first = delta == 0 and b == 0

        def tile(m, carry):
            rows = pl.ds(pl.multiple_of(m * 256, 256), 256)
            wide = quick(a_hi[b * 4 + j, rows], both, NN)
            part = wide[:, :128] + wide[:, 128:] + quick(a_lo[b * 4 + j, rows], high, NN)
            part = part.reshape(2, 128, 128)
            if first:
                yp[q, m] = part
            else:
                yp[q, m] = yp[q, m] + part
            return carry

        lax.fori_loop(0, 4, tile, 0)

    def pair_start(q):
        send(copy_to(yp.at[q, :, 1 - k], drx.at[q], d_send.at[q], d_recv.at[q],
                     dev(x, y, z, 1 - k)))

    def scatter_start(q):
        arrived(drx.at[q], d_recv.at[q])
        yh[q] = yp[q, :, k] + drx[q]
        for d in range(1, 4):
            other = (z + d) % 4
            send(copy_to(yh.at[q, other], zrx.at[q, z], zr_send.at[q, d - 1], zr_recv.at[q, z],
                         dev(x, y, other, k)))
        zrx[q, z] = yh[q, z]

    def scatter_finish(q):
        for d in range(1, 4):
            other = (z + d) % 4
            arrived(zrx.at[q, other], zr_recv.at[q, other])
        total = zrx[q, 0] + zrx[q, 1] + zrx[q, 2] + zrx[q, 3]
        ys[q] = total
        yr[q, z, k] = total
        t_start(1, q)
        for d in range(1, 4):
            send(copy_to(ys.at[q], yr.at[q, z, k], za_send.at[q, d - 1], za_recv.at[q, z],
                         dev(x, y, (z + d) % 4, k)))

    def rows_pass(q):
        for d in range(1, 4):
            other = (z + d) % 4
            arrived(yr.at[q, other, k], za_recv.at[q, other])
        half = yr.at[q, :, k]
        send(copy_to(half, half, e_send.at[q], e_recv.at[q], dev(x, y, z, 1 - k)))

    def rows_finish(q):
        arrived(yr.at[q, :, 1 - k], e_recv.at[q])

    def sum_start(g):
        for d in range(1, 4):
            send(copy_to(pb.at[g, col], xb.at[g, x], gx_send.at[g, d - 1], gx_recv.at[g, x],
                         dev((x + d) % 4, y, z, k)))
        xb[g, x] = pb[g, col]

    def sum_middle(g):
        for d in range(1, 4):
            other = (x + d) % 4
            arrived(xb.at[g, other], gx_recv.at[g, other])
        yb[g, y] = xb[g, 0] + xb[g, 1] + xb[g, 2] + xb[g, 3]
        for d in range(1, 4):
            send(copy_to(yb.at[g, y], yb.at[g, y], gy_send.at[g, d - 1], gy_recv.at[g, y],
                         dev(x, (y + d) % 4, z, k)))

    def sum_gather(g):
        for d in range(1, 4):
            other = (y + d) % 4
            arrived(yb.at[g, other], gy_recv.at[g, other])
        gb[g, col] = yb[g, 0] + yb[g, 1] + yb[g, 2] + yb[g, 3]
        for d in range(1, 8):
            send(copy_to(gb.at[g, col], gb.at[g, col], gg_send.at[g, d - 1], gg_recv.at[g, col],
                         (row, (col + d) % 8)))

    def sum_finish(g):
        for d in range(1, 8):
            other = (col + d) % 8
            arrived(gb.at[g, other], gg_recv.at[g, other])

    def own_rows(ref, j):
        return jnp.concatenate(
            [ref[0, j].reshape(256, 128), ref[1, j].reshape(256, 128)], axis=1
        )

    def inner(g, right_ref):
        def part(j, carry):
            piece = exact(own_rows(v_ref, j), own_rows(right_ref, j), TN).reshape(8, 32, 256)

            @pl.when(j == 0)
            def _():
                pb[g] = piece

            @pl.when(j > 0)
            def _():
                pb[g] = pb[g] + piece

            return carry

        lax.fori_loop(0, 4, part, 0)

    ri = lax.broadcasted_iota(jnp.int32, (256, 256), 0)
    ci = lax.broadcasted_iota(jnp.int32, (256, 256), 1)

    def eye():
        return jnp.where(ri == ci, 1.0, 0.0).astype(F32)

    def factor_start():
        gram = gb[0].reshape(256, 256)
        halves = jnp.sum(jnp.where(ri == ci, gram, 0.0), axis=0, keepdims=True) * 0.5
        block = jnp.logical_and(ri // 64 == ci // 64, ci > ri)
        negated = -(jnp.where(block, gram, 0.0) / halves)
        pw[...] = negated
        inv[...] = eye() + negated

    def factor_double():
        power = exact(pw[...], pw[...], NN)
        pw[...] = power
        inv[...] = exact(inv[...], eye() + power, NN)

    def factor_scale():
        gram = gb[0].reshape(256, 256)
        halves = jnp.sum(jnp.where(ri == ci, gram, 0.0), axis=1, keepdims=True) * 0.5
        inv[...] = inv[...] / halves

    def factor_join(width):
        gram = gb[0].reshape(256, 256)
        above = jnp.logical_and(ri // (2 * width) == ci // (2 * width), ri // width < ci // width)
        off = jnp.where(above, gram, 0.0)
        inv[...] = inv[...] - exact(exact(inv[...], off, NN), inv[...], NN)

    def write_out(plane, source, q):
        copies = []
        for b in range(2):
            copies.append(pltpu.make_async_copy(
                source.at[q, b], rc_hbm.at[plane, b], out_sem.at[plane, b]))
        for copy in copies:
            copy.start()
        return copies

    t_start(0, 0)
    t_start(0, 1)
    inner(0, v_ref)
    sum_start(0)

    for i in range(8):
        slab(i).wait()

        def chop(m, carry):
            rows = pl.ds(pl.multiple_of(m * 128, 128), 128)
            high, low = split(a_buf[i, rows])
            a_hi[i, rows] = high
            a_lo[i, rows] = low
            return carry

        lax.fori_loop(0, 8, chop, 0)
        if i == 3:
            y_start(0, 0)
            x_own(0, 0, 0)
            y_start(0, 1)
    sum_middle(0)
    for delta in DELTAS[1:]:
        x_own(0, 0, delta)
    sum_gather(0)
    for delta in DELTAS:
        for b in range(2):
            x_take(0, 0, delta, b)
        x_own(0, 1, delta)
        for b in range(2):
            multiply(0, delta, b)
    pair_start(0)
    for n, delta in enumerate(DELTAS):
        for b in range(2):
            x_take(0, 1, delta, b)
        if n == 0:
            scatter_start(0)
        for b in range(2):
            multiply(1, delta, b)
        if n == 2:
            scatter_finish(0)
    pair_start(1)
    out_copies = write_out(2, vc, 0) + write_out(3, vc, 1)
    y_start(1, 0)
    x_own(1, 0, 0)
    scatter_start(1)
    for delta in DELTAS[1:]:
        x_own(1, 0, delta)
    sum_finish(0)
    factor_start()
    factor_double()
    scatter_finish(1)
    for n, delta in enumerate(DELTAS):
        for b in range(2):
            x_take(1, 0, delta, b)
        if n == 0:
            y_start(1, 1)
            rows_pass(0)
            rows_pass(1)
        x_own(1, 1, delta)
        if n == 1:
            rows_finish(0)
            rows_finish(1)
            inner(1, yr)
            sum_start(1)
        else:
            factor_double()
        if n == 2:
            sum_middle(1)
        if n == 3:
            sum_gather(1)
    out_copies += write_out(0, yc, 0)
    for n, delta in enumerate(DELTAS):
        for b in range(2):
            x_take(1, 1, delta, b)
        if n == 0:
            factor_double()
            factor_scale()
            factor_join(64)
            factor_join(128)
        if n == 1:
            sum_finish(1)
            moved = exact(gb[1].reshape(256, 256), inv[...], NN)
            mm[...] = exact(inv[...], moved, TN)
        if n == 2:
            def left(j, carry):
                rows = pl.ds(pl.multiple_of(j * 256, 256), 256)
                v_rows = own_rows(v_ref, j)
                high, low = split(exact(v_rows, inv[...], NT))
                lhi_ref[rows, :256] = high
                llo_ref[rows, :256] = low
                other = exact(own_rows(yr, j), inv[...], NN) - exact(v_rows, mm[...], NN)
                high, low = split(other)
                lhi_ref[rows, 256:] = high
                llo_ref[rows, 256:] = low
                return carry

            lax.fori_loop(0, 4, left, 0)
    out_copies += write_out(1, yc, 1)

    for copy, cond in sent:
        if cond is None:
            copy.wait_send()
        else:
            pl.when(cond)(copy.wait_send)
    for copy in out_copies:
        copy.wait()


def exchange(trailing, panels):
    dma = pltpu.SemaphoreType.DMA
    return pl.pallas_call(
        exchange_kernel,
        out_shape=(
            jax.ShapeDtypeStruct((1024, 512), BF16),
            jax.ShapeDtypeStruct((1024, 512), BF16),
            jax.ShapeDtypeStruct((4, 2, 4, 2, 128, 128), F32),
        ),
        in_specs=[
            pl.BlockSpec(memory_space=pl.ANY),
            pl.BlockSpec(memory_space=pltpu.VMEM),
        ],
        out_specs=(
            pl.BlockSpec(memory_space=pltpu.VMEM),
            pl.BlockSpec(memory_space=pltpu.VMEM),
            pl.BlockSpec(memory_space=pl.ANY),
        ),
        scratch_shapes=[
            pltpu.VMEM((8, 1024, 256), F32),
            pltpu.VMEM((8, 1024, 256), BF16),
            pltpu.VMEM((8, 1024, 256), BF16),
            pltpu.VMEM((2, 2, 4, 2, 128, 128), F32),
            pltpu.VMEM((2, 2, 4, 2, 128, 128), F32),
            pltpu.VMEM((2, 4, 2, 128, 128), F32),
            pltpu.VMEM((2, 4, 128, 128), F32),
            pltpu.VMEM((2, 4, 128, 128), F32),
            pltpu.VMEM((2, 4, 128, 128), F32),
            pltpu.VMEM((2, 128, 128), F32),
            pltpu.VMEM((2, 4, 2, 128, 128), F32),
            pltpu.VMEM((2, 8, 32, 256), F32),
            pltpu.VMEM((2, 4, 32, 256), F32),
            pltpu.VMEM((2, 4, 32, 256), F32),
            pltpu.VMEM((2, 8, 32, 256), F32),
            pltpu.VMEM((256, 256), F32),
            pltpu.VMEM((256, 256), F32),
            pltpu.VMEM((256, 256), F32),
            dma((8,)),
            dma((4, 2)),
            dma((2, 2)),
            dma((2, 2, 2)),
            dma((2, 2, 3)),
            dma((2, 2, 4)),
            dma((2, 2, 3, 4, 2)),
            dma((2, 2, 2, 4)),
            dma((2,)),
            dma((2,)),
            dma((2, 3)),
            dma((2, 4)),
            dma((2, 3)),
            dma((2, 4)),
            dma((2,)),
            dma((2,)),
            dma((2, 3)),
            dma((2, 4)),
            dma((2, 3)),
            dma((2, 4)),
            dma((2, 7)),
            dma((2, 8)),
        ],
        compiler_params=pltpu.CompilerParams(
            collective_id=0, has_side_effects=True, vmem_limit_bytes=60 * 1024 * 1024
        ),
        cost_estimate=pl.CostEstimate(
            flops=4_000_000_000, bytes_accessed=16 * 1024 * 1024, transcendentals=0
        ),
        name="exchange",
    )(trailing, panels)


def update_kernel(a_ref, lhi_ref, llo_ref, r_ref, o_ref):
    right = jnp.concatenate([r_ref[n].reshape(256, 128) for n in range(4)], axis=1)
    high, low = split(right)

    def tile(m, carry):
        rows = pl.ds(pl.multiple_of(m * 256, 256), 256)
        left_high = lhi_ref[rows]
        part = quick(left_high, high, NT) + quick(left_high, low, NT)
        part = part + quick(llo_ref[rows], high, NT)
        o_ref[rows] = a_ref[rows] - part
        return carry

    lax.fori_loop(0, 4, tile, 0)


def update(trailing, left_high, left_low, right):
    return pl.pallas_call(
        update_kernel,
        grid=(8,),
        out_shape=jax.ShapeDtypeStruct(trailing.shape, F32),
        in_specs=[
            pl.BlockSpec((1024, 256), lambda i: (0, i)),
            pl.BlockSpec((1024, 512), lambda i: (0, 0)),
            pl.BlockSpec((1024, 512), lambda i: (0, 0)),
            pl.BlockSpec((4, 1, 1, 2, 128, 128), lambda i: (0, i // 4, i % 4, 0, 0, 0)),
        ],
        out_specs=pl.BlockSpec((1024, 256), lambda i: (0, i)),
        compiler_params=pltpu.CompilerParams(vmem_limit_bytes=40 * 1024 * 1024),
        name="update",
    )(trailing, left_high, left_low, right)


def local(trailing, reflectors):
    local_rows = trailing.shape[0]
    panels = unit_lower(reflectors, lax.axis_index("row") * local_rows)
    panels = jnp.concatenate([panels[0::2], panels[1::2]], axis=2)
    panels = panels.reshape(2, 4, 2, 128, 128)
    left_high, left_low, right = exchange(trailing, panels)
    return update(trailing, left_high, left_low, right)


def solution(mesh):
    placed = (P("row", "col"), P(None, "row", None))
    return jax.shard_map(
        local, mesh=mesh, in_specs=placed, out_specs=P("row", "col"), check_vma=False
    )
```

```python
import jax
import jax.numpy as jnp
from jax import lax
from jax.experimental import pallas as pl
from jax.experimental.pallas import tpu as pltpu
from jax.sharding import PartitionSpec as P

MESH = pl.DeviceIdType.MESH
F32 = jnp.float32
BF16 = jnp.bfloat16
TILE = 512


def exact(left, right, dims):
    return lax.dot_general(
        left, right, (dims, ((), ())), precision=lax.Precision.HIGHEST, preferred_element_type=F32
    )


def quick(left, right, dims):
    return lax.dot_general(left, right, (dims, ((), ())), preferred_element_type=F32)


def split(value):
    high = value.astype(BF16)
    low = (value - high.astype(F32)).astype(BF16)
    return high, low


NN = ((1,), (0,))
NT = ((1,), (1,))


def exchange_kernel(
    a_hbm, raw_ref,
    lhi_ref, llo_ref, rc_hbm,
    a_buf, a_hi, a_lo, vt, vr, vc, yc, yp, drx, yh, zrx, ys, yr,
    pb, xb, yb, gb, pw, inv, mm,
    a_sem, out_sem,
    t_send, t_recv, p_send, p_recv,
    d_send, d_recv, zr_send, zr_recv, za_send, za_recv, e_send, e_recv,
    gx_send, gx_recv, gy_send, gy_recv, gg_send, gg_recv,
):
    row = lax.axis_index("row")
    col = lax.axis_index("col")
    x, y = row % 4, row // 4
    z, k = col // 2, col % 2

    def dev(dx, dy, dz, dk):
        return (dy * 4 + dx, dz * 2 + dk)

    def copy_to(src, dst, send, recv, device):
        return pltpu.make_async_remote_copy(
            src_ref=src, dst_ref=dst, send_sem=send, recv_sem=recv,
            device_id=device, device_id_type=MESH,
        )

    def arrived(dst, recv):
        copy_to(dst, dst, recv, recv, dev(x, y, z, 1 - k)).wait_recv()

    sent = []

    def send(copy, cond=None):
        if cond is None:
            copy.start()
        else:
            pl.when(cond)(copy.start)
        sent.append((copy, cond))

    is_src = k == x // 2
    b_own = x % 2
    stays = jnp.logical_and(y == z, is_src)

    def slab(i):
        return pltpu.make_async_copy(
            a_hbm.at[:, pl.ds(i * 256, 256)], a_buf.at[i], a_sem.at[i]
        )

    for i in range(8):
        slab(i).start()

    barrier = pltpu.get_barrier_semaphore()

    def greet(device):
        pl.semaphore_signal(barrier, inc=1, device_id=device, device_id_type=MESH)

    for d in range(1, 4):
        greet(dev((x + d) % 4, y, z, k))
        greet(dev(x, (y + d) % 4, z, k))
    for d in range(1, 8):
        greet((row, (col + d) % 8))

    @pl.when(y != z)
    def _():
        greet(dev(x, z, y, 0))
        greet(dev(x, z, y, 1))

    for n in range(8):
        for q in range(2):
            piece = raw_ref[q * 128:(q + 1) * 128, n * 128:(n + 1) * 128]
            here = row * 1024 + n * 128 + lax.broadcasted_iota(jnp.int32, (128, 128), 1)
            pivot = (q * 128 + 64) + lax.broadcasted_iota(jnp.int32, (128, 128), 0)
            ones_part = jnp.where(here == pivot, 1.0, 0.0).astype(F32)
            piece = jnp.where(here > pivot, piece, ones_part)
            vt[q * 128:(q + 1) * 128, n * 128:(n + 1) * 128] = piece
            vr[q, n // 4, n % 4] = piece.T

    pl.semaphore_wait(barrier, jnp.where(y != z, 15, 13))

    def t_start(ph, q):
        target = vc if ph == 0 else yc
        source = vr.at[q, k, z] if ph == 0 else ys.at[q]
        place = target.at[q, b_own, k, z]
        send(
            copy_to(source, place, t_send.at[ph, q], t_recv.at[ph, q, k], dev(x, z, y, x // 2)),
            jnp.logical_not(stays),
        )

        @pl.when(stays)
        def _():
            if ph == 0:
                vc[q, b_own, k, z] = vr[q, k, z]
            else:
                yc[q, b_own, k, z] = ys[q]

    def spread(ph, q, slot, b, h, j, along_x, cond):
        piece = (vc if ph == 0 else yc).at[q, b, h, j]
        for d in range(1, 4):
            device = dev((x + d) % 4, y, z, k) if along_x else dev(x, (y + d) % 4, z, k)
            send(
                copy_to(piece, piece, p_send.at[ph, q, slot, d - 1], p_recv.at[ph, q, b, h, j],
                        device),
                cond,
            )

    def piece_in(ph, q, b, h, j, cond):
        @pl.when(cond)
        def _():
            arrived((vc if ph == 0 else yc).at[q, b, h, j], p_recv.at[ph, q, b, h, j])

    def step_a(ph, q):
        target = vc if ph == 0 else yc
        for h in range(2):
            @pl.when(jnp.logical_and(
                is_src, jnp.logical_not(jnp.logical_and(y == z, k == h))))
            def _():
                arrived(target.at[q, b_own, h, y], t_recv.at[ph, q, h])

            spread(ph, q, 2 * h, b_own, h, y, h == 1, is_src)
            spread(ph, q, 2 * h + 1, b_own, h, y, h == 0, is_src)

    def step_b(ph, q):
        for n, delta in enumerate((1, 3, 2)):
            j = (y + 4 - delta) % 4
            piece_in(ph, q, b_own, 0, j, is_src)
            spread(ph, q, 4 + n, b_own, 0, j, True, is_src)

    def foreign(b):
        return jnp.logical_not(jnp.logical_and(is_src, b_own == b))

    def step_c(ph, q):
        for b in range(2):
            piece_in(ph, q, b, 1, y, foreign(b))
            spread(ph, q, 7 + b, b, 1, y, False, foreign(b))

    def step_d(ph, q, b, h, jp):
        for j in (2 * jp, 2 * jp + 1):
            piece_in(ph, q, b, h, j, foreign(b) if h == 0 else y != j)

    def multiply(q, b, h, jp):
        high, low = split(vc[q, b, h, 2 * jp:2 * jp + 2].reshape(256, 128))
        both = jnp.concatenate([high, low], axis=1)
        i = b * 4 + h * 2 + jp

        def tile(m, carry):
            rows = pl.ds(pl.multiple_of(m * 256, 256), 256)
            wide = quick(a_hi[i, rows], both, NN)
            part = wide[:, :128] + wide[:, 128:] + quick(a_lo[i, rows], high, NN)
            part = part.reshape(2, 128, 128)
            place = (q, m // 2, pl.ds(2 * (m % 2), 2))
            if i == 0:
                yp[place] = part
            else:
                yp[place] = yp[place] + part
            return carry

        lax.fori_loop(0, 4, tile, 0)

    def pair_start(q):
        send(copy_to(yp.at[q, 1 - k], drx.at[q], d_send.at[q], d_recv.at[q],
                     dev(x, y, z, 1 - k)))

    def scatter_start(q):
        arrived(drx.at[q], d_recv.at[q])
        yh[q] = yp[q, k] + drx[q]
        for d in range(1, 4):
            other = (z + d) % 4
            send(copy_to(yh.at[q, other], zrx.at[q, z], zr_send.at[q, d - 1], zr_recv.at[q, z],
                         dev(x, y, other, k)))
        zrx[q, z] = yh[q, z]

    def scatter_finish(q):
        for d in range(1, 4):
            other = (z + d) % 4
            arrived(zrx.at[q, other], zr_recv.at[q, other])
        total = zrx[q, 0] + zrx[q, 1] + zrx[q, 2] + zrx[q, 3]
        ys[q] = total
        yr[q, k, z] = total
        t_start(1, q)
        for d in range(1, 4):
            send(copy_to(ys.at[q], yr.at[q, k, z], za_send.at[q, d - 1], za_recv.at[q, z],
                         dev(x, y, (z + d) % 4, k)))

    def rows_pass(q):
        for d in range(1, 4):
            other = (z + d) % 4
            arrived(yr.at[q, k, other], za_recv.at[q, other])
        half = yr.at[q, k]
        send(copy_to(half, half, e_send.at[q], e_recv.at[q], dev(x, y, z, 1 - k)))

    def rows_finish(q):
        arrived(yr.at[q, 1 - k], e_recv.at[q])

    def sum_start(g):
        for d in range(1, 4):
            send(copy_to(pb.at[g, col], xb.at[g, x], gx_send.at[g, d - 1], gx_recv.at[g, x],
                         dev((x + d) % 4, y, z, k)))
        xb[g, x] = pb[g, col]

    def sum_middle(g):
        for d in range(1, 4):
            other = (x + d) % 4
            arrived(xb.at[g, other], gx_recv.at[g, other])
        yb[g, y] = xb[g, 0] + xb[g, 1] + xb[g, 2] + xb[g, 3]
        for d in range(1, 4):
            send(copy_to(yb.at[g, y], yb.at[g, y], gy_send.at[g, d - 1], gy_recv.at[g, y],
                         dev(x, (y + d) % 4, z, k)))

    def sum_gather(g):
        for d in range(1, 4):
            other = (y + d) % 4
            arrived(yb.at[g, other], gy_recv.at[g, other])
        gb[g, col] = yb[g, 0] + yb[g, 1] + yb[g, 2] + yb[g, 3]
        for d in range(1, 8):
            send(copy_to(gb.at[g, col], gb.at[g, col], gg_send.at[g, d - 1], gg_recv.at[g, col],
                         (row, (col + d) % 8)))

    def sum_finish(g):
        for d in range(1, 8):
            other = (col + d) % 8
            arrived(gb.at[g, other], gg_recv.at[g, other])

    def own_rows(ref, m):
        here = (m // 2, pl.ds(2 * (m % 2), 2))
        return jnp.concatenate(
            [ref[(0,) + here].reshape(256, 128), ref[(1,) + here].reshape(256, 128)], axis=1
        )

    def inner(g, right_ref):
        def part(m, carry):
            left_part = vt[:, pl.ds(pl.multiple_of(m * 256, 256), 256)]
            piece = exact(left_part, own_rows(right_ref, m), NN).reshape(8, 32, 256)

            @pl.when(m == 0)
            def _():
                pb[g] = piece

            @pl.when(m > 0)
            def _():
                pb[g] = pb[g] + piece

            return carry

        lax.fori_loop(0, 4, part, 0)

    ri = lax.broadcasted_iota(jnp.int32, (256, 256), 0)
    ci = lax.broadcasted_iota(jnp.int32, (256, 256), 1)

    def eye():
        return jnp.where(ri == ci, 1.0, 0.0).astype(F32)

    def factor_start():
        gram = gb[0].reshape(256, 256)
        halves = jnp.sum(jnp.where(ri == ci, gram, 0.0), axis=0, keepdims=True) * 0.5
        block = jnp.logical_and(ri // 64 == ci // 64, ci > ri)
        negated = -(jnp.where(block, gram, 0.0) / halves)
        pw[...] = negated
        inv[...] = eye() + negated

    def factor_double(step, carry):
        power = exact(pw[...], pw[...], NN)
        pw[...] = power
        inv[...] = exact(inv[...], eye() + power, NN)
        return carry

    def factor_scale():
        gram = gb[0].reshape(256, 256)
        halves = jnp.sum(jnp.where(ri == ci, gram, 0.0), axis=1, keepdims=True) * 0.5
        inv[...] = inv[...] / halves

    def factor_join(width):
        gram = gb[0].reshape(256, 256)
        above = jnp.logical_and(ri // (2 * width) == ci // (2 * width), ri // width < ci // width)
        off = jnp.where(above, gram, 0.0)
        inv[...] = inv[...] - exact(exact(inv[...], off, NN), inv[...], NN)

    out_copies = []

    def write_out(plane, source, q, b, h):
        copy = pltpu.make_async_copy(
            source.at[q, b, h], rc_hbm.at[plane, b, h], out_sem.at[plane, b, h])
        copy.start()
        out_copies.append(copy)

    units = [(b, h, jp) for b in range(2) for h in range(2) for jp in range(2)]

    t_start(0, 0)
    t_start(0, 1)
    inner(0, vr)
    sum_start(0)
    step_a(0, 0)

    for i in range(8):
        slab(i).wait()

        def chop(m, carry):
            rows = pl.ds(pl.multiple_of(m * 128, 128), 128)
            high, low = split(a_buf[i, rows])
            a_hi[i, rows] = high
            a_lo[i, rows] = low
            return carry

        lax.fori_loop(0, 8, chop, 0)
    step_b(0, 0)
    step_c(0, 0)
    step_a(0, 1)
    sum_middle(0)
    for n, (b, h, jp) in enumerate(units):
        step_d(0, 0, b, h, jp)
        multiply(0, b, h, jp)
        if n == 1:
            step_b(0, 1)
            step_c(0, 1)
            sum_gather(0)
    pair_start(0)
    for n, (b, h, jp) in enumerate(units):
        step_d(0, 1, b, h, jp)
        multiply(1, b, h, jp)
        if n == 2:
            scatter_start(0)
        if n == 6:
            scatter_finish(0)
    pair_start(1)
    for q in range(2):
        for b in range(2):
            for h in range(2):
                write_out(2 + q, vc, q, b, h)
    step_a(1, 0)
    scatter_start(1)
    sum_finish(0)
    step_b(1, 0)
    step_c(1, 0)
    factor_start()
    scatter_finish(1)
    rows_pass(0)
    lax.fori_loop(0, 5, factor_double, 0)
    step_a(1, 1)
    rows_pass(1)
    factor_scale()
    factor_join(64)
    factor_join(128)
    rows_finish(0)
    rows_finish(1)
    step_b(1, 1)
    step_c(1, 1)
    inner(1, yr)
    sum_start(1)

    def left_panel(m, carry):
        rows = pl.ds(pl.multiple_of(m * 256, 256), 256)
        high, low = split(exact(own_rows(vr, m), inv[...], NT))
        lhi_ref[rows, :256] = high
        llo_ref[rows, :256] = low
        return carry

    lax.fori_loop(0, 4, left_panel, 0)
    sum_middle(1)
    for b, h, jp in units:
        step_d(1, 0, b, h, jp)
        if jp == 1:
            write_out(0, yc, 0, b, h)
    sum_gather(1)
    sum_finish(1)
    mm[...] = exact(inv[...].T, exact(gb[1].reshape(256, 256), inv[...], NN), NN)

    def left_update(m, carry):
        rows = pl.ds(pl.multiple_of(m * 256, 256), 256)
        other = exact(own_rows(yr, m), inv[...], NN) - exact(own_rows(vr, m), mm[...], NN)
        high, low = split(other)
        lhi_ref[rows, 256:] = high
        llo_ref[rows, 256:] = low
        return carry

    lax.fori_loop(0, 4, left_update, 0)
    for b, h, jp in units:
        step_d(1, 1, b, h, jp)
        if jp == 1:
            write_out(1, yc, 1, b, h)

    for copy, cond in sent:
        if cond is None:
            copy.wait_send()
        else:
            pl.when(cond)(copy.wait_send)
    for copy in out_copies:
        copy.wait()


def exchange(trailing, raw):
    dma = pltpu.SemaphoreType.DMA
    pieces = pltpu.VMEM((2, 2, 2, 4, 128, 128), F32)
    by_rows = pltpu.VMEM((2, 2, 4, 128, 128), F32)
    halves = pltpu.VMEM((2, 4, 128, 128), F32)
    whole = pltpu.VMEM((2, 8, 32, 256), F32)
    slices = pltpu.VMEM((2, 4, 32, 256), F32)
    square = pltpu.VMEM((256, 256), F32)
    return pl.pallas_call(
        exchange_kernel,
        out_shape=(
            jax.ShapeDtypeStruct((1024, 512), BF16),
            jax.ShapeDtypeStruct((1024, 512), BF16),
            jax.ShapeDtypeStruct((4, 2, 2, 4, 128, 128), F32),
        ),
        in_specs=[
            pl.BlockSpec(memory_space=pl.ANY),
            pl.BlockSpec(memory_space=pltpu.VMEM),
        ],
        out_specs=(
            pl.BlockSpec(memory_space=pltpu.VMEM),
            pl.BlockSpec(memory_space=pltpu.VMEM),
            pl.BlockSpec(memory_space=pl.ANY),
        ),
        scratch_shapes=[
            pltpu.VMEM((8, 1024, 256), F32),
            pltpu.VMEM((8, 1024, 256), BF16),
            pltpu.VMEM((8, 1024, 256), BF16),
            pltpu.VMEM((256, 1024), F32),
            by_rows, pieces, pieces, by_rows, halves, halves, halves,
            pltpu.VMEM((2, 128, 128), F32),
            by_rows, whole, slices, slices, whole, square, square, square,
            dma((8,)),
            dma((4, 2, 2)),
            dma((2, 2)),
            dma((2, 2, 2)),
            dma((2, 2, 9, 3)),
            dma((2, 2, 2, 2, 4)),
            dma((2,)),
            dma((2,)),
            dma((2, 3)),
            dma((2, 4)),
            dma((2, 3)),
            dma((2, 4)),
            dma((2,)),
            dma((2,)),
            dma((2, 3)),
            dma((2, 4)),
            dma((2, 3)),
            dma((2, 4)),
            dma((2, 7)),
            dma((2, 8)),
        ],
        compiler_params=pltpu.CompilerParams(
            collective_id=0, has_side_effects=True, vmem_limit_bytes=60 * 1024 * 1024
        ),
        cost_estimate=pl.CostEstimate(
            flops=4_000_000_000, bytes_accessed=16 * 1024 * 1024, transcendentals=0
        ),
        name="exchange",
    )(trailing, raw)


def update_kernel(a_ref, lhi_ref, llo_ref, r_ref, o_ref):
    right = jnp.concatenate([r_ref[n].reshape(256, 128) for n in range(4)], axis=1)
    high, low = split(right)
    right = jnp.concatenate([high, low, high], axis=1)

    def tile(m, carry):
        rows = pl.ds(pl.multiple_of(m * TILE, TILE), TILE)
        left_high = lhi_ref[rows]
        left = jnp.concatenate([left_high, left_high, llo_ref[rows]], axis=1)
        o_ref[rows] = a_ref[rows] - quick(left, right, NT)
        return carry

    lax.fori_loop(0, 1024 // TILE, tile, 0)


def update(trailing, left_high, left_low, right):
    return pl.pallas_call(
        update_kernel,
        grid=(8,),
        out_shape=jax.ShapeDtypeStruct(trailing.shape, F32),
        in_specs=[
            pl.BlockSpec((1024, 256), lambda i: (0, i)),
            pl.BlockSpec((1024, 512), lambda i: (0, 0)),
            pl.BlockSpec((1024, 512), lambda i: (0, 0)),
            pl.BlockSpec((4, 1, 1, 2, 128, 128), lambda i: (0, i // 4, i // 2 % 2, i % 2, 0, 0)),
        ],
        out_specs=pl.BlockSpec((1024, 256), lambda i: (0, i)),
        compiler_params=pltpu.CompilerParams(vmem_limit_bytes=62 * 1024 * 1024),
        name="update",
    )(trailing, left_high, left_low, right)


def local(trailing, reflectors):
    raw = jnp.swapaxes(reflectors, 1, 2).reshape(256, 1024)
    left_high, left_low, right = exchange(trailing, raw)
    return update(trailing, left_high, left_low, right)


def solution(mesh):
    placed = (P("row", "col"), P(None, "row", None))
    return jax.shard_map(
        local, mesh=mesh, in_specs=placed, out_specs=P("row", "col"), check_vma=False
    )
```

```python
import jax
import jax.numpy as jnp
from jax import lax
from jax.experimental import pallas as pl
from jax.experimental.pallas import tpu as pltpu
from jax.sharding import PartitionSpec as P

MESH = pl.DeviceIdType.MESH
F32 = jnp.float32
BF16 = jnp.bfloat16


def exact(left, right, dims):
    return lax.dot_general(
        left, right, (dims, ((), ())), precision=lax.Precision.HIGHEST, preferred_element_type=F32
    )


def quick(left, right, dims):
    return lax.dot_general(left, right, (dims, ((), ())), preferred_element_type=F32)


def split(value):
    high = value.astype(BF16)
    low = (value - high.astype(F32)).astype(BF16)
    return high, low


NN = ((1,), (0,))
NT = ((1,), (1,))


def exchange_kernel(
    a_hbm, raw_ref,
    out_ref,
    a_buf, a_hi, a_lo, vt, vr, vc, yc, yp, drx, yh, zrx, ys, yr,
    pb, cb, xb, yb, gb, pw, inv, mm, lhi_ref, llo_ref,
    a_sem,
    t_send, t_recv, p_send, p_recv,
    d_send, d_recv, zr_send, zr_recv, za_send, za_recv, e_send, e_recv,
    gc_send, gc_recv, gx_send, gx_recv, gy_send, gy_recv, gg_send, gg_recv,
):
    row = lax.axis_index("row")
    col = lax.axis_index("col")
    x, y = row % 4, row // 4
    z, k = col // 2, col % 2

    def dev(dx, dy, dz, dk):
        return (dy * 4 + dx, dz * 2 + dk)

    def copy_to(src, dst, send, recv, device):
        return pltpu.make_async_remote_copy(
            src_ref=src, dst_ref=dst, send_sem=send, recv_sem=recv,
            device_id=device, device_id_type=MESH,
        )

    def arrived(dst, recv):
        copy_to(dst, dst, recv, recv, dev(x, y, z, 1 - k)).wait_recv()

    sent = []

    def send(copy, cond=None):
        if cond is None:
            copy.start()
        else:
            pl.when(cond)(copy.start)
        sent.append((copy, cond))

    is_src = k == x // 2
    b_own = x % 2
    stays = jnp.logical_and(y == z, is_src)

    def slab(i):
        return pltpu.make_async_copy(
            a_hbm.at[:, pl.ds(i * 256, 256)], a_buf.at[i], a_sem.at[i]
        )

    for i in range(8):
        slab(i).start()

    barrier = pltpu.get_barrier_semaphore()

    def greet(device):
        pl.semaphore_signal(barrier, inc=1, device_id=device, device_id_type=MESH)

    for d in range(1, 4):
        greet(dev((x + d) % 4, y, z, k))
        greet(dev(x, (y + d) % 4, z, k))
    for d in range(1, 8):
        greet((row, (col + d) % 8))

    @pl.when(y != z)
    def _():
        greet(dev(x, z, y, 0))
        greet(dev(x, z, y, 1))

    for n in range(8):
        for q in range(2):
            piece = raw_ref[q * 128:(q + 1) * 128, n * 128:(n + 1) * 128]
            here = row * 1024 + n * 128 + lax.broadcasted_iota(jnp.int32, (128, 128), 1)
            pivot = (q * 128 + 64) + lax.broadcasted_iota(jnp.int32, (128, 128), 0)
            ones_part = jnp.where(here == pivot, 1.0, 0.0).astype(F32)
            piece = jnp.where(here > pivot, piece, ones_part)
            vt[q * 128:(q + 1) * 128, n * 128:(n + 1) * 128] = piece
            vr[q, n // 4, n % 4] = piece.T

    pl.semaphore_wait(barrier, jnp.where(y != z, 15, 13))

    def t_start(ph, q):
        target = vc if ph == 0 else yc
        source = vr.at[q, k, z] if ph == 0 else ys.at[q]
        place = target.at[q, b_own, k, z]
        send(
            copy_to(source, place, t_send.at[ph, q], t_recv.at[ph, q, k], dev(x, z, y, x // 2)),
            jnp.logical_not(stays),
        )

        @pl.when(stays)
        def _():
            if ph == 0:
                vc[q, b_own, k, z] = vr[q, k, z]
            else:
                yc[q, b_own, k, z] = ys[q]

    def spread(ph, q, slot, b, h, j, along_x, cond):
        piece = (vc if ph == 0 else yc).at[q, b, h, j]
        for d in range(1, 4):
            device = dev((x + d) % 4, y, z, k) if along_x else dev(x, (y + d) % 4, z, k)
            send(
                copy_to(piece, piece, p_send.at[ph, q, slot, d - 1], p_recv.at[ph, q, b, h, j],
                        device),
                cond,
            )

    def piece_in(ph, q, b, h, j, cond):
        @pl.when(cond)
        def _():
            arrived((vc if ph == 0 else yc).at[q, b, h, j], p_recv.at[ph, q, b, h, j])

    def step_a(ph, q):
        target = vc if ph == 0 else yc
        for h in range(2):
            @pl.when(jnp.logical_and(
                is_src, jnp.logical_not(jnp.logical_and(y == z, k == h))))
            def _():
                arrived(target.at[q, b_own, h, y], t_recv.at[ph, q, h])

            spread(ph, q, 2 * h, b_own, h, y, h == 1, is_src)
            spread(ph, q, 2 * h + 1, b_own, h, y, h == 0, is_src)

    def step_b(ph, q):
        for n, delta in enumerate((1, 3, 2)):
            j = (y + 4 - delta) % 4
            piece_in(ph, q, b_own, 0, j, is_src)
            spread(ph, q, 4 + n, b_own, 0, j, True, is_src)

    def foreign(b):
        return jnp.logical_not(jnp.logical_and(is_src, b_own == b))

    def step_c(ph, q):
        for b in range(2):
            piece_in(ph, q, b, 1, y, foreign(b))
            spread(ph, q, 7 + b, b, 1, y, False, foreign(b))

    def step_d(ph, q, b, h, j):
        piece_in(ph, q, b, h, j, jnp.logical_or(
            jnp.logical_and(h == 0, foreign(b)), jnp.logical_and(h == 1, y != j)))

    def multiply(q, t):
        b, h = (b_own + t // 2) % 2, t % 2
        for j in range(4):
            step_d(0, q, b, h, j)
        high, low = split(vc[q, b, h].reshape(512, 128))
        both = jnp.concatenate([high, low], axis=1)
        i = b * 4 + h * 2

        def tile(m, carry):
            rows = pl.ds(pl.multiple_of(m * 512, 512), 512)
            wide = quick(jnp.concatenate([a_hi[i, rows], a_hi[i + 1, rows]], axis=1), both, NN)
            slim = quick(jnp.concatenate([a_lo[i, rows], a_lo[i + 1, rows]], axis=1), high, NN)
            part = (wide[:, :128] + wide[:, 128:] + slim).reshape(4, 128, 128)
            if t == 0:
                yp[q, m] = part
            else:
                yp[q, m] = yp[q, m] + part
            return carry

        lax.fori_loop(0, 2, tile, 0)

    def pair_start(q):
        send(copy_to(yp.at[q, 1 - k], drx.at[q], d_send.at[q], d_recv.at[q],
                     dev(x, y, z, 1 - k)))

    def scatter_start(q):
        arrived(drx.at[q], d_recv.at[q])
        yh[q] = yp[q, k] + drx[q]
        for d in range(1, 4):
            other = (z + d) % 4
            send(copy_to(yh.at[q, other], zrx.at[q, z], zr_send.at[q, d - 1], zr_recv.at[q, z],
                         dev(x, y, other, k)))
        zrx[q, z] = yh[q, z]

    def scatter_finish(q):
        for d in range(1, 4):
            other = (z + d) % 4
            arrived(zrx.at[q, other], zr_recv.at[q, other])
        total = zrx[q, 0] + zrx[q, 1] + zrx[q, 2] + zrx[q, 3]
        ys[q] = total
        yr[q, k, z] = total
        t_start(1, q)
        for d in range(1, 4):
            send(copy_to(ys.at[q], yr.at[q, k, z], za_send.at[q, d - 1], za_recv.at[q, z],
                         dev(x, y, (z + d) % 4, k)))

    def rows_pass(q):
        for d in range(1, 4):
            other = (z + d) % 4
            arrived(yr.at[q, k, other], za_recv.at[q, other])
        half = yr.at[q, k]
        send(copy_to(half, half, e_send.at[q], e_recv.at[q], dev(x, y, z, 1 - k)))

    def rows_finish(q):
        arrived(yr.at[q, 1 - k], e_recv.at[q])

    def column_start():
        for d in range(1, 8):
            other = (col + d) % 8
            send(copy_to(pb.at[1, other], cb.at[col], gc_send.at[d - 1], gc_recv.at[col],
                         (row, other)))
        cb[col] = pb[1, col]

    def column_finish():
        for d in range(1, 8):
            other = (col + d) % 8
            arrived(cb.at[other], gc_recv.at[other])
        total = cb[0]
        for n in range(1, 8):
            total = total + cb[n]
        xb[1, x] = total

    def sum_start(g):
        for d in range(1, 4):
            send(copy_to(xb.at[g, x], xb.at[g, x], gx_send.at[g, d - 1], gx_recv.at[g, x],
                         dev((x + d) % 4, y, z, k)))

    def sum_middle(g):
        for d in range(1, 4):
            other = (x + d) % 4
            arrived(xb.at[g, other], gx_recv.at[g, other])
        yb[g, y] = xb[g, 0] + xb[g, 1] + xb[g, 2] + xb[g, 3]
        for d in range(1, 4):
            send(copy_to(yb.at[g, y], yb.at[g, y], gy_send.at[g, d - 1], gy_recv.at[g, y],
                         dev(x, (y + d) % 4, z, k)))

    def sum_gather(g):
        for d in range(1, 4):
            other = (y + d) % 4
            arrived(yb.at[g, other], gy_recv.at[g, other])
        gb[g, col] = yb[g, 0] + yb[g, 1] + yb[g, 2] + yb[g, 3]
        for d in range(1, 8):
            send(copy_to(gb.at[g, col], gb.at[g, col], gg_send.at[g, d - 1], gg_recv.at[g, col],
                         (row, (col + d) % 8)))

    def sum_finish(g):
        for d in range(1, 8):
            other = (col + d) % 8
            arrived(gb.at[g, other], gg_recv.at[g, other])

    def own_rows(ref, m):
        here = (m // 2, pl.ds(2 * (m % 2), 2))
        return jnp.concatenate(
            [ref[(0,) + here].reshape(256, 128), ref[(1,) + here].reshape(256, 128)], axis=1
        )

    def inner(g, right_ref):
        def part(m, carry):
            left_part = vt[:, pl.ds(pl.multiple_of(m * 256, 256), 256)]
            piece = exact(left_part, own_rows(right_ref, m), NN).reshape(8, 32, 256)

            @pl.when(m == 0)
            def _():
                pb[g] = piece

            @pl.when(m > 0)
            def _():
                pb[g] = pb[g] + piece

            return carry

        lax.fori_loop(0, 4, part, 0)

    ri = lax.broadcasted_iota(jnp.int32, (256, 256), 0)
    ci = lax.broadcasted_iota(jnp.int32, (256, 256), 1)

    def eye():
        return jnp.where(ri == ci, 1.0, 0.0).astype(F32)

    def factor_start():
        gram = gb[0].reshape(256, 256)
        halves = jnp.sum(jnp.where(ri == ci, gram, 0.0), axis=0, keepdims=True) * 0.5
        block = jnp.logical_and(ri // 64 == ci // 64, ci > ri)
        negated = -(jnp.where(block, gram, 0.0) / halves)
        pw[...] = negated
        inv[...] = eye() + negated

    def factor_double(step, carry):
        power = exact(pw[...], pw[...], NN)
        pw[...] = power
        inv[...] = exact(inv[...], eye() + power, NN)
        return carry

    def factor_scale():
        gram = gb[0].reshape(256, 256)
        halves = jnp.sum(jnp.where(ri == ci, gram, 0.0), axis=1, keepdims=True) * 0.5
        inv[...] = inv[...] / halves

    def factor_join(width):
        gram = gb[0].reshape(256, 256)
        above = jnp.logical_and(ri // (2 * width) == ci // (2 * width), ri // width < ci // width)
        off = jnp.where(above, gram, 0.0)
        inv[...] = inv[...] - exact(exact(inv[...], off, NN), inv[...], NN)

    def place(t):
        b, n = (b_own + t // 4) % 2, t % 4
        h = (n + 1) // 2 % 2
        jp = h * (n - 1) + (1 - h) * ((y // 2 + n // 3) % 2)
        return b, h, jp

    def finish(t, carry):
        b, h, jp = place(t)
        for q in range(2):
            for n in range(2):
                step_d(1, q, b, h, 2 * jp + n)
        here = (b, h, pl.ds(2 * jp, 2))
        right = jnp.concatenate(
            [ref[(q,) + here].reshape(256, 128) for ref in (yc, vc) for q in range(2)], axis=1
        )
        high, low = split(right)
        right = jnp.concatenate([high, low, high], axis=1)
        i = b * 4 + h * 2 + jp

        def tile(m, inside):
            rows = pl.ds(pl.multiple_of(m * 512, 512), 512)
            left_high = lhi_ref[rows]
            left = jnp.concatenate([left_high, left_high, llo_ref[rows]], axis=1)
            columns = pl.ds(pl.multiple_of(i * 256, 256), 256)
            out_ref[rows, columns] = a_buf[i, rows] - quick(left, right, NT)
            return inside

        lax.fori_loop(0, 2, tile, 0)
        return carry

    t_start(0, 0)
    t_start(0, 1)
    inner(0, vr)
    xb[0, x] = pb[0, col]
    sum_start(0)
    step_a(0, 0)

    for i in range(8):
        slab(i).wait()

        def chop(m, carry):
            rows = pl.ds(pl.multiple_of(m * 128, 128), 128)
            high, low = split(a_buf[i, rows])
            a_hi[i, rows] = high
            a_lo[i, rows] = low
            return carry

        lax.fori_loop(0, 8, chop, 0)
    step_b(0, 0)
    step_c(0, 0)
    step_a(0, 1)
    sum_middle(0)
    for t in range(4):
        multiply(0, t)
        if t == 1:
            step_b(0, 1)
            step_c(0, 1)
            sum_gather(0)
    pair_start(0)
    for t in range(4):
        multiply(1, t)
        if t == 0:
            scatter_start(0)
        if t == 2:
            scatter_finish(0)
    pair_start(1)
    inner(1, yp)
    column_start()
    step_a(1, 0)
    scatter_start(1)
    column_finish()
    sum_start(1)
    step_b(1, 0)
    sum_middle(1)
    step_c(1, 0)
    scatter_finish(1)
    sum_finish(0)
    factor_start()
    lax.fori_loop(0, 5, factor_double, 0)
    sum_gather(1)
    factor_scale()
    factor_join(64)
    factor_join(128)
    step_a(1, 1)
    rows_pass(0)
    rows_pass(1)

    def left_panel(m, carry):
        rows = pl.ds(pl.multiple_of(m * 256, 256), 256)
        high, low = split(exact(own_rows(vr, m), inv[...], NT))
        lhi_ref[rows, :256] = high
        llo_ref[rows, :256] = low
        return carry

    lax.fori_loop(0, 4, left_panel, 0)
    step_b(1, 1)
    step_c(1, 1)
    rows_finish(0)
    rows_finish(1)
    sum_finish(1)
    mm[...] = exact(inv[...].T, exact(gb[1].reshape(256, 256), inv[...], NN), NN)

    def left_update(m, carry):
        rows = pl.ds(pl.multiple_of(m * 256, 256), 256)
        other = exact(own_rows(yr, m), inv[...], NN) - exact(own_rows(vr, m), mm[...], NN)
        high, low = split(other)
        lhi_ref[rows, 256:] = high
        llo_ref[rows, 256:] = low
        return carry

    lax.fori_loop(0, 4, left_update, 0)
    lax.fori_loop(0, 8, finish, 0)

    for copy, cond in sent:
        if cond is None:
            copy.wait_send()
        else:
            pl.when(cond)(copy.wait_send)


def exchange(trailing, raw):
    dma = pltpu.SemaphoreType.DMA
    pieces = pltpu.VMEM((2, 2, 2, 4, 128, 128), F32)
    by_rows = pltpu.VMEM((2, 2, 4, 128, 128), F32)
    halves = pltpu.VMEM((2, 4, 128, 128), F32)
    whole = pltpu.VMEM((2, 8, 32, 256), F32)
    slices = pltpu.VMEM((2, 4, 32, 256), F32)
    square = pltpu.VMEM((256, 256), F32)
    left = pltpu.VMEM((1024, 512), BF16)
    return pl.pallas_call(
        exchange_kernel,
        out_shape=jax.ShapeDtypeStruct(trailing.shape, F32),
        in_specs=[
            pl.BlockSpec(memory_space=pl.ANY),
            pl.BlockSpec(memory_space=pltpu.VMEM),
        ],
        out_specs=pl.BlockSpec(memory_space=pltpu.VMEM),
        scratch_shapes=[
            pltpu.VMEM((8, 1024, 256), F32),
            pltpu.VMEM((8, 1024, 256), BF16),
            pltpu.VMEM((8, 1024, 256), BF16),
            pltpu.VMEM((256, 1024), F32),
            by_rows, pieces, pieces, by_rows, halves, halves, halves,
            pltpu.VMEM((2, 128, 128), F32),
            by_rows, whole, pltpu.VMEM((8, 32, 256), F32), slices, slices, whole,
            square, square, square, left, left,
            dma((8,)),
            dma((2, 2)),
            dma((2, 2, 2)),
            dma((2, 2, 9, 3)),
            dma((2, 2, 2, 2, 4)),
            dma((2,)),
            dma((2,)),
            dma((2, 3)),
            dma((2, 4)),
            dma((2, 3)),
            dma((2, 4)),
            dma((2,)),
            dma((2,)),
            dma((7,)),
            dma((8,)),
            dma((2, 3)),
            dma((2, 4)),
            dma((2, 3)),
            dma((2, 4)),
            dma((2, 7)),
            dma((2, 8)),
        ],
        compiler_params=pltpu.CompilerParams(
            collective_id=0, has_side_effects=True, vmem_limit_bytes=44 * 1024 * 1024
        ),
        cost_estimate=pl.CostEstimate(
            flops=8_000_000_000, bytes_accessed=16 * 1024 * 1024, transcendentals=0
        ),
        name="exchange",
    )(trailing, raw)


def local(trailing, reflectors):
    raw = jnp.swapaxes(reflectors, 1, 2).reshape(256, 1024)
    return exchange(trailing, raw)


def solution(mesh):
    placed = (P("row", "col"), P(None, "row", None))
    return jax.shard_map(
        local, mesh=mesh, in_specs=placed, out_specs=P("row", "col"), check_vma=False
    )
```

```python
import jax
import jax.numpy as jnp
from jax import lax
from jax.experimental import pallas as pl
from jax.experimental.pallas import tpu as pltpu
from jax.sharding import PartitionSpec as P

MESH = pl.DeviceIdType.MESH
F32 = jnp.float32
BF16 = jnp.bfloat16


def exact(left, right, dims):
    return lax.dot_general(
        left, right, (dims, ((), ())), precision=lax.Precision.HIGHEST, preferred_element_type=F32
    )


def quick(left, right, dims):
    return lax.dot_general(left, right, (dims, ((), ())), preferred_element_type=F32)


def split(value):
    high = value.astype(BF16)
    low = (value - high.astype(F32)).astype(BF16)
    return high, low


NN = ((1,), (0,))
NT = ((1,), (1,))


def exchange_kernel(
    a_hbm, raw_ref,
    out_ref,
    a_buf, a_hi, a_lo, vt, vr, vc, yc, yp, drx, yh, zrx, ys, yr,
    pb, sb, cb, xb, yb, gb, pw, inv, mm, lhi_ref, llo_ref,
    a_sem,
    t_send, t_recv, p_send, p_recv,
    d_send, d_recv, zr_send, zr_recv, za_send, za_recv, e_send, e_recv,
    gc_send, gc_recv, gx_send, gx_recv, gy_send, gy_recv, gg_send, gg_recv,
):
    row = lax.axis_index("row")
    col = lax.axis_index("col")
    x, y = row % 4, row // 4
    z, k = col // 2, col % 2

    def dev(dx, dy, dz, dk):
        return (dy * 4 + dx, dz * 2 + dk)

    def copy_to(src, dst, send, recv, device):
        return pltpu.make_async_remote_copy(
            src_ref=src, dst_ref=dst, send_sem=send, recv_sem=recv,
            device_id=device, device_id_type=MESH,
        )

    def arrived(dst, recv):
        copy_to(dst, dst, recv, recv, dev(x, y, z, 1 - k)).wait_recv()

    sent = []

    def send(copy, cond=None):
        if cond is None:
            copy.start()
        else:
            pl.when(cond)(copy.start)
        sent.append((copy, cond))

    is_src = k == x // 2
    b_own = x % 2
    stays = jnp.logical_and(y == z, is_src)

    def slab(i):
        return pltpu.make_async_copy(
            a_hbm.at[:, pl.ds(i * 256, 256)], a_buf.at[i], a_sem.at[i]
        )

    for i in range(8):
        slab(i).start()

    barrier = pltpu.get_barrier_semaphore()

    def greet(device):
        pl.semaphore_signal(barrier, inc=1, device_id=device, device_id_type=MESH)

    for d in range(1, 4):
        greet(dev((x + d) % 4, y, z, k))
        greet(dev(x, (y + d) % 4, z, k))
    for d in range(1, 8):
        greet((row, (col + d) % 8))

    @pl.when(y != z)
    def _():
        greet(dev(x, z, y, 0))
        greet(dev(x, z, y, 1))

    for n in range(8):
        for q in range(2):
            piece = raw_ref[q * 128:(q + 1) * 128, n * 128:(n + 1) * 128]
            here = row * 1024 + n * 128 + lax.broadcasted_iota(jnp.int32, (128, 128), 1)
            pivot = (q * 128 + 64) + lax.broadcasted_iota(jnp.int32, (128, 128), 0)
            ones_part = jnp.where(here == pivot, 1.0, 0.0).astype(F32)
            piece = jnp.where(here > pivot, piece, ones_part)
            vt[q * 128:(q + 1) * 128, n * 128:(n + 1) * 128] = piece
            vr[q, n // 4, n % 4] = piece.T

    pl.semaphore_wait(barrier, jnp.where(y != z, 15, 13))

    def t_start(ph, q):
        target = vc if ph == 0 else yc
        source = vr.at[q, k, z] if ph == 0 else ys.at[q]
        place = target.at[q, b_own, k, z]
        send(
            copy_to(source, place, t_send.at[ph, q], t_recv.at[ph, q, k], dev(x, z, y, x // 2)),
            jnp.logical_not(stays),
        )

        @pl.when(stays)
        def _():
            if ph == 0:
                vc[q, b_own, k, z] = vr[q, k, z]
            else:
                yc[q, b_own, k, z] = ys[q]

    def spread(ph, q, slot, b, h, j, along_x, cond):
        piece = (vc if ph == 0 else yc).at[q, b, h, j]
        for d in range(1, 4):
            device = dev((x + d) % 4, y, z, k) if along_x else dev(x, (y + d) % 4, z, k)
            send(
                copy_to(piece, piece, p_send.at[ph, q, slot, d - 1], p_recv.at[ph, q, b, h, j],
                        device),
                cond,
            )

    def piece_in(ph, q, b, h, j, cond):
        @pl.when(cond)
        def _():
            arrived((vc if ph == 0 else yc).at[q, b, h, j], p_recv.at[ph, q, b, h, j])

    def step_a(ph, q):
        target = vc if ph == 0 else yc
        for h in range(2):
            @pl.when(jnp.logical_and(
                is_src, jnp.logical_not(jnp.logical_and(y == z, k == h))))
            def _():
                arrived(target.at[q, b_own, h, y], t_recv.at[ph, q, h])

            spread(ph, q, 2 * h, b_own, h, y, h == 1, is_src)
            spread(ph, q, 2 * h + 1, b_own, h, y, h == 0, is_src)

    def step_b(ph, q):
        for n, delta in enumerate((1, 3, 2)):
            j = (y + 4 - delta) % 4
            piece_in(ph, q, b_own, 0, j, is_src)
            spread(ph, q, 4 + n, b_own, 0, j, True, is_src)

    def foreign(b):
        return jnp.logical_not(jnp.logical_and(is_src, b_own == b))

    def step_c(ph, q):
        for b in range(2):
            piece_in(ph, q, b, 1, y, foreign(b))
            spread(ph, q, 7 + b, b, 1, y, False, foreign(b))

    def step_d(ph, q, b, h, j):
        piece_in(ph, q, b, h, j, jnp.logical_or(
            jnp.logical_and(h == 0, foreign(b)), jnp.logical_and(h == 1, y != j)))

    def multiply(q, t):
        b, h = (b_own + t // 2) % 2, t % 2
        for j in range(4):
            step_d(0, q, b, h, j)
        high, low = split(vc[q, b, h].reshape(512, 128))
        both = jnp.concatenate([high, low], axis=1)
        i = b * 4 + h * 2

        def tile(m, carry):
            rows = pl.ds(pl.multiple_of(m * 512, 512), 512)
            wide = quick(jnp.concatenate([a_hi[i, rows], a_hi[i + 1, rows]], axis=1), both, NN)
            slim = quick(jnp.concatenate([a_lo[i, rows], a_lo[i + 1, rows]], axis=1), high, NN)
            part = (wide[:, :128] + wide[:, 128:] + slim).reshape(4, 128, 128)
            if t == 0:
                yp[q, m] = part
            else:
                yp[q, m] = yp[q, m] + part
            return carry

        lax.fori_loop(0, 2, tile, 0)

    def pair_start(q):
        send(copy_to(yp.at[q, 1 - k], drx.at[q], d_send.at[q], d_recv.at[q],
                     dev(x, y, z, 1 - k)))

    def scatter_start(q):
        arrived(drx.at[q], d_recv.at[q])
        yh[q] = yp[q, k] + drx[q]
        for d in range(1, 4):
            other = (z + d) % 4
            send(copy_to(yh.at[q, other], zrx.at[q, z], zr_send.at[q, d - 1], zr_recv.at[q, z],
                         dev(x, y, other, k)))
        zrx[q, z] = yh[q, z]

    def scatter_finish(q):
        for d in range(1, 4):
            other = (z + d) % 4
            arrived(zrx.at[q, other], zr_recv.at[q, other])
        total = zrx[q, 0] + zrx[q, 1] + zrx[q, 2] + zrx[q, 3]
        ys[q] = total
        yr[q, k, z] = total
        t_start(1, q)
        for d in range(1, 4):
            send(copy_to(ys.at[q], yr.at[q, k, z], za_send.at[q, d - 1], za_recv.at[q, z],
                         dev(x, y, (z + d) % 4, k)))

    def rows_pass(q):
        for d in range(1, 4):
            other = (z + d) % 4
            arrived(yr.at[q, k, other], za_recv.at[q, other])
        half = yr.at[q, k]
        send(copy_to(half, half, e_send.at[q], e_recv.at[q], dev(x, y, z, 1 - k)))

    def rows_finish(q):
        arrived(yr.at[q, 1 - k], e_recv.at[q])

    def column_start(q):
        for d in range(1, 8):
            other = (col + d) % 8
            send(copy_to(sb.at[q, other], cb.at[q, col], gc_send.at[q, d - 1], gc_recv.at[q, col],
                         (row, other)))
        cb[q, col] = sb[q, col]

    def column_finish(q):
        for d in range(1, 8):
            other = (col + d) % 8
            arrived(cb.at[q, other], gc_recv.at[q, other])
        total = cb[q, 0]
        for n in range(1, 8):
            total = total + cb[q, n]
        xb[1, x, :, q * 128:(q + 1) * 128] = total

    def sum_start(g):
        for d in range(1, 4):
            send(copy_to(xb.at[g, x], xb.at[g, x], gx_send.at[g, d - 1], gx_recv.at[g, x],
                         dev((x + d) % 4, y, z, k)))

    def sum_middle(g):
        for d in range(1, 4):
            other = (x + d) % 4
            arrived(xb.at[g, other], gx_recv.at[g, other])
        yb[g, y] = xb[g, 0] + xb[g, 1] + xb[g, 2] + xb[g, 3]
        for d in range(1, 4):
            send(copy_to(yb.at[g, y], yb.at[g, y], gy_send.at[g, d - 1], gy_recv.at[g, y],
                         dev(x, (y + d) % 4, z, k)))

    def sum_gather(g):
        for d in range(1, 4):
            other = (y + d) % 4
            arrived(yb.at[g, other], gy_recv.at[g, other])
        gb[g, col] = yb[g, 0] + yb[g, 1] + yb[g, 2] + yb[g, 3]
        for d in range(1, 8):
            send(copy_to(gb.at[g, col], gb.at[g, col], gg_send.at[g, d - 1], gg_recv.at[g, col],
                         (row, (col + d) % 8)))

    def sum_finish(g):
        for d in range(1, 8):
            other = (col + d) % 8
            arrived(gb.at[g, other], gg_recv.at[g, other])

    def own_rows(ref, m):
        here = (m // 2, pl.ds(2 * (m % 2), 2))
        return jnp.concatenate(
            [ref[(0,) + here].reshape(256, 128), ref[(1,) + here].reshape(256, 128)], axis=1
        )

    def inner(target, right_of):
        def part(m, carry):
            left_part = vt[:, pl.ds(pl.multiple_of(m * 256, 256), 256)]
            piece = exact(left_part, right_of(m), NN).reshape(target.shape)

            @pl.when(m == 0)
            def _():
                target[...] = piece

            @pl.when(m > 0)
            def _():
                target[...] = target[...] + piece

            return carry

        lax.fori_loop(0, 4, part, 0)

    def product_rows(q):
        return lambda m: yp[q, m // 2, pl.ds(2 * (m % 2), 2)].reshape(256, 128)

    ri = lax.broadcasted_iota(jnp.int32, (256, 256), 0)
    ci = lax.broadcasted_iota(jnp.int32, (256, 256), 1)

    def eye():
        return jnp.where(ri == ci, 1.0, 0.0).astype(F32)

    def factor_start():
        gram = gb[0].reshape(256, 256)
        halves = jnp.sum(jnp.where(ri == ci, gram, 0.0), axis=0, keepdims=True) * 0.5
        block = jnp.logical_and(ri // 64 == ci // 64, ci > ri)
        negated = -(jnp.where(block, gram, 0.0) / halves)
        pw[...] = negated
        inv[...] = eye() + negated

    def factor_double(step, carry):
        power = exact(pw[...], pw[...], NN)
        pw[...] = power
        inv[...] = exact(inv[...], eye() + power, NN)
        return carry

    def factor_scale():
        gram = gb[0].reshape(256, 256)
        halves = jnp.sum(jnp.where(ri == ci, gram, 0.0), axis=1, keepdims=True) * 0.5
        inv[...] = inv[...] / halves

    def factor_join(width):
        gram = gb[0].reshape(256, 256)
        above = jnp.logical_and(ri // (2 * width) == ci // (2 * width), ri // width < ci // width)
        off = jnp.where(above, gram, 0.0)
        inv[...] = inv[...] - exact(exact(inv[...], off, NN), inv[...], NN)

    def place(t):
        b, n = (b_own + t // 4) % 2, t % 4
        h = (n + 1) // 2 % 2
        jp = h * (n - 1) + (1 - h) * ((y // 2 + n // 3) % 2)
        return b, h, jp

    def finish(t, carry):
        b, h, jp = place(t)
        for q in range(2):
            for n in range(2):
                step_d(1, q, b, h, 2 * jp + n)
        here = (b, h, pl.ds(2 * jp, 2))
        right = jnp.concatenate(
            [ref[(q,) + here].reshape(256, 128) for ref in (yc, vc) for q in range(2)], axis=1
        )
        high, low = split(right)
        right = jnp.concatenate([high, low, high], axis=1)
        i = b * 4 + h * 2 + jp

        def tile(m, inside):
            rows = pl.ds(pl.multiple_of(m * 512, 512), 512)
            left_high = lhi_ref[rows]
            left = jnp.concatenate([left_high, left_high, llo_ref[rows]], axis=1)
            columns = pl.ds(pl.multiple_of(i * 256, 256), 256)
            out_ref[rows, columns] = a_buf[i, rows] - quick(left, right, NT)
            return inside

        lax.fori_loop(0, 2, tile, 0)
        return carry

    t_start(0, 0)
    t_start(0, 1)
    inner(pb, lambda m: own_rows(vr, m))
    xb[0, x] = pb[col]
    sum_start(0)
    step_a(0, 0)

    for i in range(8):
        slab(i).wait()

        def chop(m, carry):
            rows = pl.ds(pl.multiple_of(m * 128, 128), 128)
            high, low = split(a_buf[i, rows])
            a_hi[i, rows] = high
            a_lo[i, rows] = low
            return carry

        lax.fori_loop(0, 8, chop, 0)
    step_b(0, 0)
    step_c(0, 0)
    step_a(0, 1)
    sum_middle(0)
    for t in range(4):
        multiply(0, t)
        if t == 1:
            step_b(0, 1)
            step_c(0, 1)
            sum_gather(0)
    pair_start(0)
    inner(sb.at[0], product_rows(0))
    scatter_start(0)
    column_start(0)
    sum_finish(0)
    factor_start()
    lax.fori_loop(0, 5, factor_double, 0)
    multiply(1, 0)
    factor_scale()
    factor_join(64)
    factor_join(128)
    multiply(1, 1)
    scatter_finish(0)
    multiply(1, 2)
    column_finish(0)
    multiply(1, 3)
    pair_start(1)
    inner(sb.at[1], product_rows(1))
    column_start(1)
    scatter_start(1)
    step_a(1, 0)
    column_finish(1)
    sum_start(1)
    step_b(1, 0)
    rows_pass(0)
    sum_middle(1)
    scatter_finish(1)
    step_c(1, 0)

    def left_panel(m, carry):
        rows = pl.ds(pl.multiple_of(m * 256, 256), 256)
        high, low = split(exact(own_rows(vr, m), inv[...], NT))
        lhi_ref[rows, :256] = high
        llo_ref[rows, :256] = low
        return carry

    lax.fori_loop(0, 4, left_panel, 0)
    sum_gather(1)
    step_a(1, 1)
    rows_pass(1)
    step_b(1, 1)
    step_c(1, 1)
    rows_finish(0)
    rows_finish(1)
    sum_finish(1)
    mm[...] = exact(inv[...].T, exact(gb[1].reshape(256, 256), inv[...], NN), NN)

    def left_update(m, carry):
        rows = pl.ds(pl.multiple_of(m * 256, 256), 256)
        other = exact(own_rows(yr, m), inv[...], NN) - exact(own_rows(vr, m), mm[...], NN)
        high, low = split(other)
        lhi_ref[rows, 256:] = high
        llo_ref[rows, 256:] = low
        return carry

    lax.fori_loop(0, 4, left_update, 0)
    lax.fori_loop(0, 8, finish, 0)

    for copy, cond in sent:
        if cond is None:
            copy.wait_send()
        else:
            pl.when(cond)(copy.wait_send)


def exchange(trailing, raw):
    dma = pltpu.SemaphoreType.DMA
    pieces = pltpu.VMEM((2, 2, 2, 4, 128, 128), F32)
    by_rows = pltpu.VMEM((2, 2, 4, 128, 128), F32)
    halves = pltpu.VMEM((2, 4, 128, 128), F32)
    whole = pltpu.VMEM((2, 8, 32, 256), F32)
    slices = pltpu.VMEM((2, 4, 32, 256), F32)
    square = pltpu.VMEM((256, 256), F32)
    left = pltpu.VMEM((1024, 512), BF16)
    columns = pltpu.VMEM((2, 8, 32, 128), F32)
    return pl.pallas_call(
        exchange_kernel,
        out_shape=jax.ShapeDtypeStruct(trailing.shape, F32),
        in_specs=[
            pl.BlockSpec(memory_space=pl.ANY),
            pl.BlockSpec(memory_space=pltpu.VMEM),
        ],
        out_specs=pl.BlockSpec(memory_space=pltpu.VMEM),
        scratch_shapes=[
            pltpu.VMEM((8, 1024, 256), F32),
            pltpu.VMEM((8, 1024, 256), BF16),
            pltpu.VMEM((8, 1024, 256), BF16),
            pltpu.VMEM((256, 1024), F32),
            by_rows, pieces, pieces, by_rows, halves, halves, halves,
            pltpu.VMEM((2, 128, 128), F32),
            by_rows, pltpu.VMEM((8, 32, 256), F32), columns, columns, slices, slices, whole,
            square, square, square, left, left,
            dma((8,)),
            dma((2, 2)),
            dma((2, 2, 2)),
            dma((2, 2, 9, 3)),
            dma((2, 2, 2, 2, 4)),
            dma((2,)),
            dma((2,)),
            dma((2, 3)),
            dma((2, 4)),
            dma((2, 3)),
            dma((2, 4)),
            dma((2,)),
            dma((2,)),
            dma((2, 7)),
            dma((2, 8)),
            dma((2, 3)),
            dma((2, 4)),
            dma((2, 3)),
            dma((2, 4)),
            dma((2, 7)),
            dma((2, 8)),
        ],
        compiler_params=pltpu.CompilerParams(
            collective_id=0, has_side_effects=True, vmem_limit_bytes=44 * 1024 * 1024
        ),
        cost_estimate=pl.CostEstimate(
            flops=8_000_000_000, bytes_accessed=16 * 1024 * 1024, transcendentals=0
        ),
        name="exchange",
    )(trailing, raw)


def local(trailing, reflectors):
    raw = jnp.swapaxes(reflectors, 1, 2).reshape(256, 1024)
    return exchange(trailing, raw)


def solution(mesh):
    placed = (P("row", "col"), P(None, "row", None))
    return jax.shard_map(
        local, mesh=mesh, in_specs=placed, out_specs=P("row", "col"), check_vma=False
    )
```

```python
import jax
import jax.numpy as jnp
from jax import lax
from jax.experimental import pallas as pl
from jax.experimental.pallas import tpu as pltpu
from jax.sharding import PartitionSpec as P

MESH = pl.DeviceIdType.MESH
F32 = jnp.float32
BF16 = jnp.bfloat16


def exact(left, right, dims):
    return lax.dot_general(
        left, right, (dims, ((), ())), precision=lax.Precision.HIGHEST, preferred_element_type=F32
    )


def quick(left, right, dims):
    return lax.dot_general(left, right, (dims, ((), ())), preferred_element_type=F32)


def split(value):
    high = value.astype(BF16)
    low = (value - high.astype(F32)).astype(BF16)
    return high, low


NN = ((1,), (0,))
NT = ((1,), (1,))


def exchange_kernel(
    a_hbm, raw_ref,
    out_ref,
    a_buf, a_hi, a_lo, vt, vr, vc, yc, yp, drx, yh, zrx, ys, yr,
    pb, sb, cb, xb, yb, gb, pw, inv, tm, lhi_ref, llo_ref, vhi_ref, vlo_ref,
    a_sem,
    t_send, t_recv, p_send, p_recv,
    d_send, d_recv, zr_send, zr_recv, za_send, za_recv, e_send, e_recv,
    gc_send, gc_recv, gx_send, gx_recv, gy_send, gy_recv, gg_send, gg_recv,
):
    row = lax.axis_index("row")
    col = lax.axis_index("col")
    x, y = row % 4, row // 4
    z, k = col // 2, col % 2

    def dev(dx, dy, dz, dk):
        return (dy * 4 + dx, dz * 2 + dk)

    def copy_to(src, dst, send, recv, device):
        return pltpu.make_async_remote_copy(
            src_ref=src, dst_ref=dst, send_sem=send, recv_sem=recv,
            device_id=device, device_id_type=MESH,
        )

    def arrived(dst, recv):
        copy_to(dst, dst, recv, recv, dev(x, y, z, 1 - k)).wait_recv()

    sent = []

    def send(copy, cond=None):
        if cond is None:
            copy.start()
        else:
            pl.when(cond)(copy.start)
        sent.append((copy, cond))

    is_src = k == x // 2
    b_own = x % 2
    stays = jnp.logical_and(y == z, is_src)

    def slab(i):
        return pltpu.make_async_copy(
            a_hbm.at[:, pl.ds(i * 256, 256)], a_buf.at[i], a_sem.at[i]
        )

    for i in range(8):
        slab(i).start()

    barrier = pltpu.get_barrier_semaphore()

    def greet(device):
        pl.semaphore_signal(barrier, inc=1, device_id=device, device_id_type=MESH)

    for d in range(1, 4):
        greet(dev((x + d) % 4, y, z, k))
        greet(dev(x, (y + d) % 4, z, k))
    for d in range(1, 8):
        greet((row, (col + d) % 8))

    @pl.when(y != z)
    def _():
        greet(dev(x, z, y, 0))
        greet(dev(x, z, y, 1))

    for n in range(8):
        for q in range(2):
            piece = raw_ref[q * 128:(q + 1) * 128, n * 128:(n + 1) * 128]
            here = row * 1024 + n * 128 + lax.broadcasted_iota(jnp.int32, (128, 128), 1)
            pivot = (q * 128 + 64) + lax.broadcasted_iota(jnp.int32, (128, 128), 0)
            ones_part = jnp.where(here == pivot, 1.0, 0.0).astype(F32)
            piece = jnp.where(here > pivot, piece, ones_part)
            vt[q * 128:(q + 1) * 128, n * 128:(n + 1) * 128] = piece
            vr[q, n // 4, n % 4] = piece.T

    pl.semaphore_wait(barrier, jnp.where(y != z, 15, 13))

    def t_start(ph, q):
        target = vc if ph == 0 else yc
        source = vr.at[q, k, z] if ph == 0 else ys.at[q]
        place = target.at[q, b_own, k, z]
        send(
            copy_to(source, place, t_send.at[ph, q], t_recv.at[ph, q, k], dev(x, z, y, x // 2)),
            jnp.logical_not(stays),
        )

        @pl.when(stays)
        def _():
            if ph == 0:
                vc[q, b_own, k, z] = vr[q, k, z]
            else:
                yc[q, b_own, k, z] = ys[q]

    def spread(ph, q, slot, b, h, j, along_x, cond):
        piece = (vc if ph == 0 else yc).at[q, b, h, j]
        for d in range(1, 4):
            device = dev((x + d) % 4, y, z, k) if along_x else dev(x, (y + d) % 4, z, k)
            send(
                copy_to(piece, piece, p_send.at[ph, q, slot, d - 1], p_recv.at[ph, q, b, h, j],
                        device),
                cond,
            )

    def piece_in(ph, q, b, h, j, cond):
        @pl.when(cond)
        def _():
            arrived((vc if ph == 0 else yc).at[q, b, h, j], p_recv.at[ph, q, b, h, j])

    def step_a(ph, q):
        target = vc if ph == 0 else yc
        for h in range(2):
            @pl.when(jnp.logical_and(
                is_src, jnp.logical_not(jnp.logical_and(y == z, k == h))))
            def _():
                arrived(target.at[q, b_own, h, y], t_recv.at[ph, q, h])

            spread(ph, q, 2 * h, b_own, h, y, h == 1, is_src)
            spread(ph, q, 2 * h + 1, b_own, h, y, h == 0, is_src)

    def step_b(ph, q):
        for n, delta in enumerate((1, 3, 2)):
            j = (y + 4 - delta) % 4
            piece_in(ph, q, b_own, 0, j, is_src)
            spread(ph, q, 4 + n, b_own, 0, j, True, is_src)

    def foreign(b):
        return jnp.logical_not(jnp.logical_and(is_src, b_own == b))

    def step_c(ph, q):
        for b in range(2):
            piece_in(ph, q, b, 1, y, foreign(b))
            spread(ph, q, 7 + b, b, 1, y, False, foreign(b))

    def step_d(ph, q, b, h, j):
        piece_in(ph, q, b, h, j, jnp.logical_or(
            jnp.logical_and(h == 0, foreign(b)), jnp.logical_and(h == 1, y != j)))

    def multiply(q, t):
        b, h = (b_own + t // 2) % 2, t % 2
        for j in range(4):
            step_d(0, q, b, h, j)
        high, low = split(vc[q, b, h].reshape(512, 128))
        both = jnp.concatenate([high, low], axis=1)
        i = b * 4 + h * 2

        def tile(m, carry):
            rows = pl.ds(pl.multiple_of(m * 512, 512), 512)
            wide = quick(jnp.concatenate([a_hi[i, rows], a_hi[i + 1, rows]], axis=1), both, NN)
            slim = quick(jnp.concatenate([a_lo[i, rows], a_lo[i + 1, rows]], axis=1), high, NN)
            part = (wide[:, :128] + wide[:, 128:] + slim).reshape(4, 128, 128)
            if t == 0:
                yp[q, m] = part
            else:
                yp[q, m] = yp[q, m] + part
            return carry

        lax.fori_loop(0, 2, tile, 0)

    def pair_start(q):
        send(copy_to(yp.at[q, 1 - k], drx.at[q], d_send.at[q], d_recv.at[q],
                     dev(x, y, z, 1 - k)))

    def scatter_start(q):
        arrived(drx.at[q], d_recv.at[q])
        yh[q] = yp[q, k] + drx[q]
        for d in range(1, 4):
            other = (z + d) % 4
            send(copy_to(yh.at[q, other], zrx.at[q, z], zr_send.at[q, d - 1], zr_recv.at[q, z],
                         dev(x, y, other, k)))
        zrx[q, z] = yh[q, z]

    def scatter_finish(q):
        for d in range(1, 4):
            other = (z + d) % 4
            arrived(zrx.at[q, other], zr_recv.at[q, other])
        total = zrx[q, 0] + zrx[q, 1] + zrx[q, 2] + zrx[q, 3]
        ys[q] = total
        yr[q, k, z] = total
        t_start(1, q)
        for d in range(1, 4):
            send(copy_to(ys.at[q], yr.at[q, k, z], za_send.at[q, d - 1], za_recv.at[q, z],
                         dev(x, y, (z + d) % 4, k)))

    def rows_pass(q):
        for d in range(1, 4):
            other = (z + d) % 4
            arrived(yr.at[q, k, other], za_recv.at[q, other])
        half = yr.at[q, k]
        send(copy_to(half, half, e_send.at[q], e_recv.at[q], dev(x, y, z, 1 - k)))

    def rows_finish(q):
        arrived(yr.at[q, 1 - k], e_recv.at[q])

    def column_start(q):
        for d in range(1, 8):
            other = (col + d) % 8
            send(copy_to(sb.at[q, other], cb.at[q, col], gc_send.at[q, d - 1], gc_recv.at[q, col],
                         (row, other)))
        cb[q, col] = sb[q, col]

    def column_finish(q):
        for d in range(1, 8):
            other = (col + d) % 8
            arrived(cb.at[q, other], gc_recv.at[q, other])
        total = cb[q, 0]
        for n in range(1, 8):
            total = total + cb[q, n]
        xb[1, x, :, q * 128:(q + 1) * 128] = total

    def sum_start(g):
        for d in range(1, 4):
            send(copy_to(xb.at[g, x], xb.at[g, x], gx_send.at[g, d - 1], gx_recv.at[g, x],
                         dev((x + d) % 4, y, z, k)))

    def sum_middle(g):
        for d in range(1, 4):
            other = (x + d) % 4
            arrived(xb.at[g, other], gx_recv.at[g, other])
        yb[g, y] = xb[g, 0] + xb[g, 1] + xb[g, 2] + xb[g, 3]
        for d in range(1, 4):
            send(copy_to(yb.at[g, y], yb.at[g, y], gy_send.at[g, d - 1], gy_recv.at[g, y],
                         dev(x, (y + d) % 4, z, k)))

    def sum_gather(g):
        for d in range(1, 4):
            other = (y + d) % 4
            arrived(yb.at[g, other], gy_recv.at[g, other])
        gb[g, col] = yb[g, 0] + yb[g, 1] + yb[g, 2] + yb[g, 3]
        for d in range(1, 8):
            send(copy_to(gb.at[g, col], gb.at[g, col], gg_send.at[g, d - 1], gg_recv.at[g, col],
                         (row, (col + d) % 8)))

    def sum_finish(g):
        for d in range(1, 8):
            other = (col + d) % 8
            arrived(gb.at[g, other], gg_recv.at[g, other])

    def own_rows(ref, m):
        here = (m // 2, pl.ds(2 * (m % 2), 2))
        return jnp.concatenate(
            [ref[(0,) + here].reshape(256, 128), ref[(1,) + here].reshape(256, 128)], axis=1
        )

    def inner(target, right_of):
        def part(m, carry):
            left_part = vt[:, pl.ds(pl.multiple_of(m * 256, 256), 256)]
            piece = exact(left_part, right_of(m), NN).reshape(target.shape)

            @pl.when(m == 0)
            def _():
                target[...] = piece

            @pl.when(m > 0)
            def _():
                target[...] = target[...] + piece

            return carry

        lax.fori_loop(0, 4, part, 0)

    def product_rows(q):
        return lambda m: yp[q, m // 2, pl.ds(2 * (m % 2), 2)].reshape(256, 128)

    ri = lax.broadcasted_iota(jnp.int32, (256, 256), 0)
    ci = lax.broadcasted_iota(jnp.int32, (256, 256), 1)

    def eye():
        return jnp.where(ri == ci, 1.0, 0.0).astype(F32)

    def factor_start():
        gram = gb[0].reshape(256, 256)
        halves = jnp.sum(jnp.where(ri == ci, gram, 0.0), axis=0, keepdims=True) * 0.5
        block = jnp.logical_and(ri // 64 == ci // 64, ci > ri)
        negated = -(jnp.where(block, gram, 0.0) / halves)
        pw[...] = negated
        inv[...] = eye() + negated

    def factor_double(step, carry):
        power = exact(pw[...], pw[...], NN)
        pw[...] = power
        inv[...] = exact(inv[...], eye() + power, NN)
        return carry

    def factor_scale():
        gram = gb[0].reshape(256, 256)
        halves = jnp.sum(jnp.where(ri == ci, gram, 0.0), axis=1, keepdims=True) * 0.5
        inv[...] = inv[...] / halves

    def factor_join(width):
        gram = gb[0].reshape(256, 256)
        above = jnp.logical_and(ri // (2 * width) == ci // (2 * width), ri // width < ci // width)
        off = jnp.where(above, gram, 0.0)
        inv[...] = inv[...] - exact(exact(inv[...], off, NN), inv[...], NN)

    def place(t):
        b, n = (b_own + t // 4) % 2, t % 4
        h = (n + 1) // 2 % 2
        jp = h * (n - 1) + (1 - h) * ((y // 2 + n // 3) % 2)
        return b, h, jp

    def pair(ref, here):
        return jnp.concatenate(
            [ref[(0,) + here].reshape(256, 128), ref[(1,) + here].reshape(256, 128)], axis=1
        )

    def subtract(i, high_ref, low_ref, right, store):
        high, low = split(right)
        right = jnp.concatenate([high, low, high], axis=1)

        def tile(m, inside):
            rows = pl.ds(pl.multiple_of(m * 512, 512), 512)
            left_high = high_ref[rows]
            left = jnp.concatenate([left_high, left_high, low_ref[rows]], axis=1)
            store(rows, a_buf[i, rows] - quick(left, right, NT))
            return inside

        lax.fori_loop(0, 2, tile, 0)

    def begin(i, carry):
        here = (i // 4, i // 2 % 2, pl.ds(2 * (i % 2), 2))

        def store(rows, value):
            a_buf[i, rows] = value

        subtract(i, lhi_ref, llo_ref, pair(vc, here), store)
        return carry

    def finish(t, carry):
        b, h, jp = place(t)
        for q in range(2):
            for n in range(2):
                step_d(1, q, b, h, 2 * jp + n)
        here = (b, h, pl.ds(2 * jp, 2))
        i = b * 4 + h * 2 + jp
        high, low = split(jnp.concatenate([pair(yc, here), pair(vc, here)], axis=1))
        total = quick(jnp.concatenate([high, high, low], axis=1), tm[...], NN)
        columns = pl.ds(pl.multiple_of(i * 256, 256), 256)

        def store(rows, value):
            out_ref[rows, columns] = value

        subtract(i, vhi_ref, vlo_ref, total, store)
        return carry

    t_start(0, 0)
    t_start(0, 1)
    inner(pb, lambda m: own_rows(vr, m))
    xb[0, x] = pb[col]
    sum_start(0)
    step_a(0, 0)
    sum_middle(0)

    for i in range(8):
        slab(i).wait()

        def chop(m, carry):
            rows = pl.ds(pl.multiple_of(m * 128, 128), 128)
            high, low = split(a_buf[i, rows])
            a_hi[i, rows] = high
            a_lo[i, rows] = low
            return carry

        lax.fori_loop(0, 8, chop, 0)
        if i == 3:
            step_b(0, 0)
            step_c(0, 0)
    step_a(0, 1)
    multiply(0, 0)
    multiply(0, 1)
    step_b(0, 1)
    step_c(0, 1)
    multiply(0, 2)
    multiply(0, 3)
    pair_start(0)
    sum_gather(0)
    inner(sb.at[0], product_rows(0))
    scatter_start(0)
    column_start(0)
    multiply(1, 0)
    sum_finish(0)
    factor_start()
    lax.fori_loop(0, 5, factor_double, 0)
    scatter_finish(0)
    multiply(1, 1)
    multiply(1, 2)
    multiply(1, 3)
    pair_start(1)
    inner(sb.at[1], product_rows(1))
    scatter_start(1)
    column_start(1)
    step_a(1, 0)
    factor_scale()
    factor_join(64)
    factor_join(128)
    column_finish(0)
    scatter_finish(1)
    column_finish(1)
    sum_start(1)
    step_b(1, 0)
    rows_pass(0)

    def split_rows(m, carry):
        rows = pl.ds(pl.multiple_of(m * 256, 256), 256)
        high, low = split(own_rows(vr, m))
        vhi_ref[rows] = high
        vlo_ref[rows] = low
        return carry

    lax.fori_loop(0, 4, split_rows, 0)
    sum_middle(1)
    step_a(1, 1)
    step_c(1, 0)
    rows_pass(1)
    rows_finish(0)
    sum_gather(1)
    step_b(1, 1)
    step_c(1, 1)
    rows_finish(1)

    def left_update(m, carry):
        rows = pl.ds(pl.multiple_of(m * 256, 256), 256)
        high, low = split(exact(own_rows(yr, m), inv[...], NN))
        lhi_ref[rows] = high
        llo_ref[rows] = low
        return carry

    lax.fori_loop(0, 4, left_update, 0)
    lax.fori_loop(0, 8, begin, 0)
    sum_finish(1)
    inner_factor = inv[...]
    coupling = exact(inner_factor.T, exact(gb[1].reshape(256, 256), inner_factor, NN), NN)
    high, low = split(inner_factor)
    tm[0:256] = high
    tm[512:768] = low
    tm[1024:1280] = high
    high, low = split(-coupling)
    tm[256:512] = high
    tm[768:1024] = low
    tm[1280:1536] = high
    lax.fori_loop(0, 8, finish, 0)

    for copy, cond in sent:
        if cond is None:
            copy.wait_send()
        else:
            pl.when(cond)(copy.wait_send)


def exchange(trailing, raw):
    dma = pltpu.SemaphoreType.DMA
    pieces = pltpu.VMEM((2, 2, 2, 4, 128, 128), F32)
    by_rows = pltpu.VMEM((2, 2, 4, 128, 128), F32)
    halves = pltpu.VMEM((2, 4, 128, 128), F32)
    whole = pltpu.VMEM((2, 8, 32, 256), F32)
    slices = pltpu.VMEM((2, 4, 32, 256), F32)
    square = pltpu.VMEM((256, 256), F32)
    left = pltpu.VMEM((1024, 256), BF16)
    columns = pltpu.VMEM((2, 8, 32, 128), F32)
    return pl.pallas_call(
        exchange_kernel,
        out_shape=jax.ShapeDtypeStruct(trailing.shape, F32),
        in_specs=[
            pl.BlockSpec(memory_space=pl.ANY),
            pl.BlockSpec(memory_space=pltpu.VMEM),
        ],
        out_specs=pl.BlockSpec(memory_space=pltpu.VMEM),
        scratch_shapes=[
            pltpu.VMEM((8, 1024, 256), F32),
            pltpu.VMEM((8, 1024, 256), BF16),
            pltpu.VMEM((8, 1024, 256), BF16),
            pltpu.VMEM((256, 1024), F32),
            by_rows, pieces, pieces, by_rows, halves, halves, halves,
            pltpu.VMEM((2, 128, 128), F32),
            by_rows, pltpu.VMEM((8, 32, 256), F32), columns, columns, slices, slices, whole,
            square, square, pltpu.VMEM((1536, 256), BF16), left, left, left, left,
            dma((8,)),
            dma((2, 2)),
            dma((2, 2, 2)),
            dma((2, 2, 9, 3)),
            dma((2, 2, 2, 2, 4)),
            dma((2,)),
            dma((2,)),
            dma((2, 3)),
            dma((2, 4)),
            dma((2, 3)),
            dma((2, 4)),
            dma((2,)),
            dma((2,)),
            dma((2, 7)),
            dma((2, 8)),
            dma((2, 3)),
            dma((2, 4)),
            dma((2, 3)),
            dma((2, 4)),
            dma((2, 7)),
            dma((2, 8)),
        ],
        compiler_params=pltpu.CompilerParams(
            collective_id=0, has_side_effects=True, vmem_limit_bytes=44 * 1024 * 1024
        ),
        cost_estimate=pl.CostEstimate(
            flops=8_000_000_000, bytes_accessed=16 * 1024 * 1024, transcendentals=0
        ),
        name="exchange",
    )(trailing, raw)


def local(trailing, reflectors):
    raw = jnp.swapaxes(reflectors, 1, 2).reshape(256, 1024)
    return exchange(trailing, raw)


def solution(mesh):
    placed = (P("row", "col"), P(None, "row", None))
    return jax.shard_map(
        local, mesh=mesh, in_specs=placed, out_specs=P("row", "col"), check_vma=False
    )
```

```python
import jax
import jax.numpy as jnp
from jax import lax
from jax.experimental import pallas as pl
from jax.experimental.pallas import tpu as pltpu
from jax.sharding import PartitionSpec as P

MESH = pl.DeviceIdType.MESH
F32 = jnp.float32
BF16 = jnp.bfloat16


def exact(left, right, dims):
    return lax.dot_general(
        left, right, (dims, ((), ())), precision=lax.Precision.HIGHEST, preferred_element_type=F32
    )


def quick(left, right, dims):
    return lax.dot_general(left, right, (dims, ((), ())), preferred_element_type=F32)


def split(value):
    high = value.astype(BF16)
    low = (value - high.astype(F32)).astype(BF16)
    return high, low


NN = ((1,), (0,))
NT = ((1,), (1,))


def exchange_kernel(
    a_hbm, raw_ref,
    out_ref,
    a_buf, a_hi, a_lo, vt, vr, vc, yc, yp, drx, yh, zrx, ys, yr,
    pb, sb, cb, xb, yb, gb, pw, inv, tm, lhi_ref, llo_ref, vhi_ref, vlo_ref,
    a_sem,
    t_send, t_recv, p_send, p_recv,
    d_send, d_recv, zr_send, zr_recv, za_send, za_recv, e_send, e_recv,
    gc_send, gc_recv, gx_send, gx_recv, gy_send, gy_recv, gg_send, gg_recv,
):
    row = lax.axis_index("row")
    col = lax.axis_index("col")
    x, y = row % 4, row // 4
    z, k = col // 2, col % 2

    def dev(dx, dy, dz, dk):
        return (dy * 4 + dx, dz * 2 + dk)

    def copy_to(src, dst, send, recv, device):
        return pltpu.make_async_remote_copy(
            src_ref=src, dst_ref=dst, send_sem=send, recv_sem=recv,
            device_id=device, device_id_type=MESH,
        )

    def arrived(dst, recv):
        copy_to(dst, dst, recv, recv, dev(x, y, z, 1 - k)).wait_recv()

    sent = []

    def send(copy, cond=None):
        if cond is None:
            copy.start()
        else:
            pl.when(cond)(copy.start)
        sent.append((copy, cond))

    is_src = k == x // 2
    b_own = x % 2
    stays = jnp.logical_and(y == z, is_src)

    def slab(i):
        return pltpu.make_async_copy(
            a_hbm.at[:, pl.ds(i * 256, 256)], a_buf.at[i], a_sem.at[i]
        )

    for i in range(8):
        slab(i).start()

    barrier = pltpu.get_barrier_semaphore()

    def greet(device):
        pl.semaphore_signal(barrier, inc=1, device_id=device, device_id_type=MESH)

    for d in range(1, 4):
        greet(dev((x + d) % 4, y, z, k))
        greet(dev(x, (y + d) % 4, z, 0))
        greet(dev(x, (y + d) % 4, z, 1))
    for d in range(1, 8):
        greet((row, (col + d) % 8))

    @pl.when(y != z)
    def _():
        greet(dev(x, z, y, 0))
        greet(dev(x, z, y, 1))

    for n in range(8):
        for q in range(2):
            piece = raw_ref[q * 128:(q + 1) * 128, n * 128:(n + 1) * 128]
            here = row * 1024 + n * 128 + lax.broadcasted_iota(jnp.int32, (128, 128), 1)
            pivot = (q * 128 + 64) + lax.broadcasted_iota(jnp.int32, (128, 128), 0)
            ones_part = jnp.where(here == pivot, 1.0, 0.0).astype(F32)
            piece = jnp.where(here > pivot, piece, ones_part)
            vt[q * 128:(q + 1) * 128, n * 128:(n + 1) * 128] = piece
            vr[q, n // 4, n % 4] = piece.T

    pl.semaphore_wait(barrier, jnp.where(y != z, 18, 16))

    def panel_start(q):
        for d in range(4):
            j = (y + d) % 4
            send(
                copy_to(vr.at[q, k, j], vc.at[q, b_own, k, j], t_send.at[0, q, d],
                        t_recv.at[0, q, k], dev(x, j, z, x // 2)),
                y == z if d else jnp.logical_and(y == z, jnp.logical_not(is_src)),
            )

        @pl.when(stays)
        def _():
            vc[q, b_own, k, y] = vr[q, k, y]

    def product_start(q):
        send(
            copy_to(ys.at[q], yc.at[q, b_own, k, z], t_send.at[1, q, 0], t_recv.at[1, q, k],
                    dev(x, z, y, x // 2)),
            jnp.logical_not(stays),
        )

        @pl.when(stays)
        def _():
            yc[q, b_own, k, z] = ys[q]

    def spread(ph, q, slot, b, h, j, along_x, cond):
        piece = (vc if ph == 0 else yc).at[q, b, h, j]
        for d in range(1, 4):
            device = dev((x + d) % 4, y, z, k) if along_x else dev(x, (y + d) % 4, z, k)
            send(
                copy_to(piece, piece, p_send.at[ph, q, slot, d - 1], p_recv.at[ph, q, b, h, j],
                        device),
                cond,
            )

    def piece_in(ph, q, b, h, j, cond):
        @pl.when(cond)
        def _():
            arrived((vc if ph == 0 else yc).at[q, b, h, j], p_recv.at[ph, q, b, h, j])

    def step_a(ph, q):
        target = vc if ph == 0 else yc
        for h in range(2):
            @pl.when(jnp.logical_and(
                is_src, jnp.logical_not(jnp.logical_and(y == z, k == h))))
            def _():
                arrived(target.at[q, b_own, h, y], t_recv.at[ph, q, h])

            spread(ph, q, 2 * h, b_own, h, y, h == 1, is_src)
            spread(ph, q, 2 * h + 1, b_own, h, y, h == 0, is_src)

    def step_b(ph, q):
        for n, delta in enumerate((1, 3, 2)):
            j = (y + 4 - delta) % 4
            piece_in(ph, q, b_own, 0, j, is_src)
            spread(ph, q, 4 + n, b_own, 0, j, True, is_src)

    def foreign(b):
        return jnp.logical_not(jnp.logical_and(is_src, b_own == b))

    def step_c(ph, q):
        for b in range(2):
            piece_in(ph, q, b, 1, y, foreign(b))
            spread(ph, q, 7 + b, b, 1, y, False, foreign(b))

    def step_d(ph, q, b, h, j):
        piece_in(ph, q, b, h, j, jnp.logical_or(
            jnp.logical_and(h == 0, foreign(b)), jnp.logical_and(h == 1, y != j)))

    def multiply(q, t):
        b, h = (b_own + t // 2) % 2, t % 2
        for j in range(4):
            step_d(0, q, b, h, j)
        high, low = split(vc[q, b, h].reshape(512, 128))
        both = jnp.concatenate([high, low], axis=1)
        i = b * 4 + h * 2

        def tile(m, carry):
            rows = pl.ds(pl.multiple_of(m * 512, 512), 512)
            wide = quick(jnp.concatenate([a_hi[i, rows], a_hi[i + 1, rows]], axis=1), both, NN)
            slim = quick(jnp.concatenate([a_lo[i, rows], a_lo[i + 1, rows]], axis=1), high, NN)
            part = (wide[:, :128] + wide[:, 128:] + slim).reshape(4, 128, 128)
            if t == 0:
                yp[q, m] = part
            else:
                yp[q, m] = yp[q, m] + part
            return carry

        lax.fori_loop(0, 2, tile, 0)

    def pair_start(q):
        send(copy_to(yp.at[q, 1 - k], drx.at[q], d_send.at[q], d_recv.at[q],
                     dev(x, y, z, 1 - k)))

    def scatter_start(q):
        arrived(drx.at[q], d_recv.at[q])
        yh[q] = yp[q, k] + drx[q]
        for d in range(1, 4):
            other = (z + d) % 4
            send(copy_to(yh.at[q, other], zrx.at[q, z], zr_send.at[q, d - 1], zr_recv.at[q, z],
                         dev(x, y, other, k)))
        zrx[q, z] = yh[q, z]

    def scatter_finish(q):
        for d in range(1, 4):
            other = (z + d) % 4
            arrived(zrx.at[q, other], zr_recv.at[q, other])
        total = zrx[q, 0] + zrx[q, 1] + zrx[q, 2] + zrx[q, 3]
        ys[q] = total
        yr[q, k, z] = total
        product_start(q)
        for d in range(1, 4):
            send(copy_to(ys.at[q], yr.at[q, k, z], za_send.at[q, d - 1], za_recv.at[q, z],
                         dev(x, y, (z + d) % 4, k)))

    def rows_pass(q):
        for d in range(1, 4):
            other = (z + d) % 4
            arrived(yr.at[q, k, other], za_recv.at[q, other])
        half = yr.at[q, k]
        send(copy_to(half, half, e_send.at[q], e_recv.at[q], dev(x, y, z, 1 - k)))

    def rows_finish(q):
        arrived(yr.at[q, 1 - k], e_recv.at[q])

    def column_start(q):
        for d in range(1, 8):
            other = (col + d) % 8
            send(copy_to(sb.at[q, other], cb.at[q, col], gc_send.at[q, d - 1], gc_recv.at[q, col],
                         (row, other)))
        cb[q, col] = sb[q, col]

    def column_finish(q):
        for d in range(1, 8):
            other = (col + d) % 8
            arrived(cb.at[q, other], gc_recv.at[q, other])
        total = cb[q, 0]
        for n in range(1, 8):
            total = total + cb[q, n]
        xb[1, x, :, q * 128:(q + 1) * 128] = total

    def sum_start(g):
        for d in range(1, 4):
            send(copy_to(xb.at[g, x], xb.at[g, x], gx_send.at[g, d - 1], gx_recv.at[g, x],
                         dev((x + d) % 4, y, z, k)))

    def sum_middle(g):
        for d in range(1, 4):
            other = (x + d) % 4
            arrived(xb.at[g, other], gx_recv.at[g, other])
        yb[g, y] = xb[g, 0] + xb[g, 1] + xb[g, 2] + xb[g, 3]
        for d in range(1, 4):
            send(copy_to(yb.at[g, y], yb.at[g, y], gy_send.at[g, d - 1], gy_recv.at[g, y],
                         dev(x, (y + d) % 4, z, k)))

    def sum_gather(g):
        for d in range(1, 4):
            other = (y + d) % 4
            arrived(yb.at[g, other], gy_recv.at[g, other])
        gb[g, col] = yb[g, 0] + yb[g, 1] + yb[g, 2] + yb[g, 3]
        for d in range(1, 8):
            send(copy_to(gb.at[g, col], gb.at[g, col], gg_send.at[g, d - 1], gg_recv.at[g, col],
                         (row, (col + d) % 8)))

    def sum_finish(g):
        for d in range(1, 8):
            other = (col + d) % 8
            arrived(gb.at[g, other], gg_recv.at[g, other])

    def own_rows(ref, m):
        here = (m // 2, pl.ds(2 * (m % 2), 2))
        return jnp.concatenate(
            [ref[(0,) + here].reshape(256, 128), ref[(1,) + here].reshape(256, 128)], axis=1
        )

    def inner(target, right_of):
        def part(m, carry):
            left_part = vt[:, pl.ds(pl.multiple_of(m * 256, 256), 256)]
            piece = exact(left_part, right_of(m), NN).reshape(target.shape)

            @pl.when(m == 0)
            def _():
                target[...] = piece

            @pl.when(m > 0)
            def _():
                target[...] = target[...] + piece

            return carry

        lax.fori_loop(0, 4, part, 0)

    def product_rows(q):
        return lambda m: yp[q, m // 2, pl.ds(2 * (m % 2), 2)].reshape(256, 128)

    ri = lax.broadcasted_iota(jnp.int32, (256, 256), 0)
    ci = lax.broadcasted_iota(jnp.int32, (256, 256), 1)

    def eye():
        return jnp.where(ri == ci, 1.0, 0.0).astype(F32)

    def factor_start():
        gram = gb[0].reshape(256, 256)
        halves = jnp.sum(jnp.where(ri == ci, gram, 0.0), axis=0, keepdims=True) * 0.5
        block = jnp.logical_and(ri // 64 == ci // 64, ci > ri)
        negated = -(jnp.where(block, gram, 0.0) / halves)
        pw[...] = negated
        inv[...] = eye() + negated

    def factor_double(step, carry):
        power = exact(pw[...], pw[...], NN)
        pw[...] = power
        inv[...] = exact(inv[...], eye() + power, NN)
        return carry

    def factor_scale():
        gram = gb[0].reshape(256, 256)
        halves = jnp.sum(jnp.where(ri == ci, gram, 0.0), axis=1, keepdims=True) * 0.5
        inv[...] = inv[...] / halves

    def factor_join(width):
        gram = gb[0].reshape(256, 256)
        above = jnp.logical_and(ri // (2 * width) == ci // (2 * width), ri // width < ci // width)
        off = jnp.where(above, gram, 0.0)
        inv[...] = inv[...] - exact(exact(inv[...], off, NN), inv[...], NN)

    def place(t):
        b, n = (b_own + t // 4) % 2, t % 4
        h = (n + 1) // 2 % 2
        jp = h * (n - 1) + (1 - h) * ((y // 2 + n // 3) % 2)
        return b, h, jp

    def pair(ref, here):
        return jnp.concatenate(
            [ref[(0,) + here].reshape(256, 128), ref[(1,) + here].reshape(256, 128)], axis=1
        )

    def subtract(i, high_ref, low_ref, right, store):
        high, low = split(right)
        right = jnp.concatenate([high, low, high], axis=1)

        left_high = high_ref[...]
        left = jnp.concatenate([left_high, left_high, low_ref[...]], axis=1)
        store(a_buf[i] - quick(left, right, NT))

    def begin(i, carry):
        here = (i // 4, i // 2 % 2, pl.ds(2 * (i % 2), 2))

        def store(value):
            a_buf[i] = value

        subtract(i, lhi_ref, llo_ref, pair(vc, here), store)
        return carry

    def finish(t, carry):
        b, h, jp = place(t)
        for q in range(2):
            for n in range(2):
                step_d(1, q, b, h, 2 * jp + n)
        here = (b, h, pl.ds(2 * jp, 2))
        i = b * 4 + h * 2 + jp
        high, low = split(jnp.concatenate([pair(yc, here), pair(vc, here)], axis=1))
        total = quick(jnp.concatenate([high, high, low], axis=1), tm[...], NN)
        columns = pl.ds(pl.multiple_of(i * 256, 256), 256)

        def store(value):
            out_ref[:, columns] = value

        subtract(i, vhi_ref, vlo_ref, total, store)
        return carry

    panel_start(0)
    panel_start(1)
    inner(pb, lambda m: own_rows(vr, m))
    xb[0, x] = pb[col]
    sum_start(0)
    step_a(0, 0)
    sum_middle(0)

    for i in range(8):
        slab(i).wait()

        def chop(m, carry):
            rows = pl.ds(pl.multiple_of(m * 128, 128), 128)
            high, low = split(a_buf[i, rows])
            a_hi[i, rows] = high
            a_lo[i, rows] = low
            return carry

        lax.fori_loop(0, 8, chop, 0)
        if i == 3:
            step_b(0, 0)
            step_c(0, 0)
    step_a(0, 1)
    multiply(0, 0)
    multiply(0, 1)
    step_b(0, 1)
    step_c(0, 1)
    multiply(0, 2)
    multiply(0, 3)
    pair_start(0)
    sum_gather(0)
    inner(sb.at[0], product_rows(0))
    scatter_start(0)
    column_start(0)
    multiply(1, 0)
    multiply(1, 1)
    scatter_finish(0)
    multiply(1, 2)
    multiply(1, 3)
    pair_start(1)
    inner(sb.at[1], product_rows(1))
    scatter_start(1)
    column_start(1)
    step_a(1, 0)
    sum_finish(0)
    factor_start()
    column_finish(0)
    scatter_finish(1)
    column_finish(1)
    sum_start(1)
    step_b(1, 0)
    rows_pass(0)
    lax.fori_loop(0, 5, factor_double, 0)

    def split_rows(m, carry):
        rows = pl.ds(pl.multiple_of(m * 256, 256), 256)
        high, low = split(own_rows(vr, m))
        vhi_ref[rows] = high
        vlo_ref[rows] = low
        return carry

    sum_middle(1)
    step_a(1, 1)
    step_c(1, 0)
    rows_pass(1)
    rows_finish(0)
    lax.fori_loop(0, 4, split_rows, 0)
    factor_scale()
    factor_join(64)
    factor_join(128)
    sum_gather(1)
    step_b(1, 1)
    step_c(1, 1)
    rows_finish(1)

    def left_update(m, carry):
        rows = pl.ds(pl.multiple_of(m * 256, 256), 256)
        high, low = split(exact(own_rows(yr, m), inv[...], NN))
        lhi_ref[rows] = high
        llo_ref[rows] = low
        return carry

    lax.fori_loop(0, 4, left_update, 0)
    lax.fori_loop(0, 8, begin, 0)
    sum_finish(1)
    inner_factor = inv[...]
    coupling = exact(inner_factor.T, exact(gb[1].reshape(256, 256), inner_factor, NN), NN)
    high, low = split(inner_factor)
    tm[0:256] = high
    tm[512:768] = low
    tm[1024:1280] = high
    high, low = split(-coupling)
    tm[256:512] = high
    tm[768:1024] = low
    tm[1280:1536] = high
    lax.fori_loop(0, 8, finish, 0)

    for copy, cond in sent:
        if cond is None:
            copy.wait_send()
        else:
            pl.when(cond)(copy.wait_send)


def exchange(trailing, raw):
    dma = pltpu.SemaphoreType.DMA
    pieces = pltpu.VMEM((2, 2, 2, 4, 128, 128), F32)
    by_rows = pltpu.VMEM((2, 2, 4, 128, 128), F32)
    halves = pltpu.VMEM((2, 4, 128, 128), F32)
    whole = pltpu.VMEM((2, 8, 32, 256), F32)
    slices = pltpu.VMEM((2, 4, 32, 256), F32)
    square = pltpu.VMEM((256, 256), F32)
    left = pltpu.VMEM((1024, 256), BF16)
    columns = pltpu.VMEM((2, 8, 32, 128), F32)
    return pl.pallas_call(
        exchange_kernel,
        out_shape=jax.ShapeDtypeStruct(trailing.shape, F32),
        in_specs=[
            pl.BlockSpec(memory_space=pl.ANY),
            pl.BlockSpec(memory_space=pltpu.VMEM),
        ],
        out_specs=pl.BlockSpec(memory_space=pltpu.VMEM),
        scratch_shapes=[
            pltpu.VMEM((8, 1024, 256), F32),
            pltpu.VMEM((8, 1024, 256), BF16),
            pltpu.VMEM((8, 1024, 256), BF16),
            pltpu.VMEM((256, 1024), F32),
            by_rows, pieces, pieces, by_rows, halves, halves, halves,
            pltpu.VMEM((2, 128, 128), F32),
            by_rows, pltpu.VMEM((8, 32, 256), F32), columns, columns, slices, slices, whole,
            square, square, pltpu.VMEM((1536, 256), BF16), left, left, left, left,
            dma((8,)),
            dma((2, 2, 4)),
            dma((2, 2, 2)),
            dma((2, 2, 9, 3)),
            dma((2, 2, 2, 2, 4)),
            dma((2,)),
            dma((2,)),
            dma((2, 3)),
            dma((2, 4)),
            dma((2, 3)),
            dma((2, 4)),
            dma((2,)),
            dma((2,)),
            dma((2, 7)),
            dma((2, 8)),
            dma((2, 3)),
            dma((2, 4)),
            dma((2, 3)),
            dma((2, 4)),
            dma((2, 7)),
            dma((2, 8)),
        ],
        compiler_params=pltpu.CompilerParams(
            collective_id=0, has_side_effects=True, vmem_limit_bytes=44 * 1024 * 1024
        ),
        cost_estimate=pl.CostEstimate(
            flops=8_000_000_000, bytes_accessed=16 * 1024 * 1024, transcendentals=0
        ),
        name="exchange",
    )(trailing, raw)


def local(trailing, reflectors):
    raw = jnp.swapaxes(reflectors, 1, 2).reshape(256, 1024)
    return exchange(trailing, raw)


def solution(mesh):
    placed = (P("row", "col"), P(None, "row", None))
    return jax.shard_map(
        local, mesh=mesh, in_specs=placed, out_specs=P("row", "col"), check_vma=False
    )
```

```python
import jax
import jax.numpy as jnp
from jax import lax
from jax.experimental import pallas as pl
from jax.experimental.pallas import tpu as pltpu
from jax.sharding import PartitionSpec as P

MESH = pl.DeviceIdType.MESH
F32 = jnp.float32
BF16 = jnp.bfloat16


def exact(left, right, dims):
    return lax.dot_general(
        left, right, (dims, ((), ())), precision=lax.Precision.HIGHEST, preferred_element_type=F32
    )


def quick(left, right, dims):
    return lax.dot_general(left, right, (dims, ((), ())), preferred_element_type=F32)


def split(value):
    high = value.astype(BF16)
    low = (value - high.astype(F32)).astype(BF16)
    return high, low


NN = ((1,), (0,))
NT = ((1,), (1,))


def exchange_kernel(
    a_hbm, raw_ref,
    out_ref,
    a_buf, a_hi, a_lo, vt, vr, vc, yc, yp, drx, yh, zrx, ys, yr,
    pb, sb, cb, xb, yb, gb, pw, inv, tm, lhi_ref, llo_ref, vhi_ref, vlo_ref,
    a_sem,
    t_send, t_recv, p_send, p_recv,
    d_send, d_recv, zr_send, zr_recv, za_send, za_recv, e_send, e_recv,
    gc_send, gc_recv, gx_send, gx_recv, gy_send, gy_recv, gg_send, gg_recv,
):
    row = lax.axis_index("row")
    col = lax.axis_index("col")
    x, y = row % 4, row // 4
    z, k = col // 2, col % 2

    def dev(dx, dy, dz, dk):
        return (dy * 4 + dx, dz * 2 + dk)

    def copy_to(src, dst, send, recv, device):
        return pltpu.make_async_remote_copy(
            src_ref=src, dst_ref=dst, send_sem=send, recv_sem=recv,
            device_id=device, device_id_type=MESH,
        )

    def arrived(dst, recv):
        copy_to(dst, dst, recv, recv, dev(x, y, z, 1 - k)).wait_recv()

    sent = []

    def send(copy, cond=None):
        if cond is None:
            copy.start()
        else:
            pl.when(cond)(copy.start)
        sent.append((copy, cond))

    is_src = k == x // 2
    b_own = x % 2
    stays = jnp.logical_and(y == z, is_src)

    def slab(i):
        return pltpu.make_async_copy(
            a_hbm.at[:, pl.ds(i * 256, 256)], a_buf.at[i], a_sem.at[i]
        )

    for i in range(8):
        slab(i).start()

    barrier = pltpu.get_barrier_semaphore()

    def greet(device):
        pl.semaphore_signal(barrier, inc=1, device_id=device, device_id_type=MESH)

    for d in range(1, 4):
        greet(dev((x + d) % 4, y, z, k))
        greet(dev(x, (y + d) % 4, z, 0))
        greet(dev(x, (y + d) % 4, z, 1))
    for d in range(1, 8):
        greet((row, (col + d) % 8))

    @pl.when(y != z)
    def _():
        greet(dev(x, z, y, 0))
        greet(dev(x, z, y, 1))

    for n in range(8):
        for q in range(2):
            piece = raw_ref[q * 128:(q + 1) * 128, n * 128:(n + 1) * 128]
            here = row * 1024 + n * 128 + lax.broadcasted_iota(jnp.int32, (128, 128), 1)
            pivot = (q * 128 + 64) + lax.broadcasted_iota(jnp.int32, (128, 128), 0)
            ones_part = jnp.where(here == pivot, 1.0, 0.0).astype(F32)
            piece = jnp.where(here > pivot, piece, ones_part)
            vt[q * 128:(q + 1) * 128, n * 128:(n + 1) * 128] = piece
            vr[q, n // 4, n % 4] = piece.T

    pl.semaphore_wait(barrier, jnp.where(y != z, 18, 16))

    def panel_start(q):
        for d in range(4):
            j = (y + d) % 4
            send(
                copy_to(vr.at[q, k, j], vc.at[q, b_own, k, j], t_send.at[0, q, d],
                        t_recv.at[0, q, k], dev(x, j, z, x // 2)),
                y == z if d else jnp.logical_and(y == z, jnp.logical_not(is_src)),
            )

        @pl.when(stays)
        def _():
            vc[q, b_own, k, y] = vr[q, k, y]

    def product_start(q):
        send(
            copy_to(ys.at[q], yc.at[q, b_own, k, z], t_send.at[1, q, 0], t_recv.at[1, q, k],
                    dev(x, z, y, x // 2)),
            jnp.logical_not(stays),
        )

        @pl.when(stays)
        def _():
            yc[q, b_own, k, z] = ys[q]

    def spread(ph, q, slot, b, h, j, along_x, cond):
        piece = (vc if ph == 0 else yc).at[q, b, h, j]
        for d in range(1, 4):
            device = dev((x + d) % 4, y, z, k) if along_x else dev(x, (y + d) % 4, z, k)
            send(
                copy_to(piece, piece, p_send.at[ph, q, slot, d - 1], p_recv.at[ph, q, b, h, j],
                        device),
                cond,
            )

    def piece_in(ph, q, b, h, j, cond):
        @pl.when(cond)
        def _():
            arrived((vc if ph == 0 else yc).at[q, b, h, j], p_recv.at[ph, q, b, h, j])

    def step_a(ph, q):
        target = vc if ph == 0 else yc
        for h in range(2):
            @pl.when(jnp.logical_and(
                is_src, jnp.logical_not(jnp.logical_and(y == z, k == h))))
            def _():
                arrived(target.at[q, b_own, h, y], t_recv.at[ph, q, h])

            spread(ph, q, 2 * h, b_own, h, y, h == 1, is_src)
            spread(ph, q, 2 * h + 1, b_own, h, y, h == 0, is_src)

    def step_b(ph, q):
        for n, delta in enumerate((1, 3, 2)):
            j = (y + 4 - delta) % 4
            piece_in(ph, q, b_own, 0, j, is_src)
            spread(ph, q, 4 + n, b_own, 0, j, True, is_src)

    def foreign(b):
        return jnp.logical_not(jnp.logical_and(is_src, b_own == b))

    def step_c(ph, q):
        for b in range(2):
            piece_in(ph, q, b, 1, y, foreign(b))
            spread(ph, q, 7 + b, b, 1, y, False, foreign(b))

    def step_d(ph, q, b, h, j):
        piece_in(ph, q, b, h, j, jnp.logical_or(
            jnp.logical_and(h == 0, foreign(b)), jnp.logical_and(h == 1, y != j)))

    def multiply(q, t):
        b, h = (b_own + t // 2) % 2, t % 2
        for j in range(4):
            step_d(0, q, b, h, j)
        high, low = split(vc[q, b, h].reshape(512, 128))
        both = jnp.concatenate([high, low], axis=1)
        i = b * 4 + h * 2

        def tile(m, carry):
            rows = pl.ds(pl.multiple_of(m * 512, 512), 512)
            wide = quick(jnp.concatenate([a_hi[i, rows], a_hi[i + 1, rows]], axis=1), both, NN)
            slim = quick(jnp.concatenate([a_lo[i, rows], a_lo[i + 1, rows]], axis=1), high, NN)
            part = (wide[:, :128] + wide[:, 128:] + slim).reshape(4, 128, 128)
            if t == 0:
                yp[q, m] = part
            else:
                yp[q, m] = yp[q, m] + part
            return carry

        lax.fori_loop(0, 2, tile, 0)

    def pair_start(q):
        send(copy_to(yp.at[q, 1 - k], drx.at[q], d_send.at[q], d_recv.at[q],
                     dev(x, y, z, 1 - k)))

    def scatter_start(q):
        arrived(drx.at[q], d_recv.at[q])
        yh[q] = yp[q, k] + drx[q]
        for d in range(1, 4):
            other = (z + d) % 4
            send(copy_to(yh.at[q, other], zrx.at[q, z], zr_send.at[q, d - 1], zr_recv.at[q, z],
                         dev(x, y, other, k)))
        zrx[q, z] = yh[q, z]

    def scatter_finish(q):
        for d in range(1, 4):
            other = (z + d) % 4
            arrived(zrx.at[q, other], zr_recv.at[q, other])
        total = zrx[q, 0] + zrx[q, 1] + zrx[q, 2] + zrx[q, 3]
        ys[q] = total
        yr[q, k, z] = total
        product_start(q)
        for d in range(1, 4):
            send(copy_to(ys.at[q], yr.at[q, k, z], za_send.at[q, d - 1], za_recv.at[q, z],
                         dev(x, y, (z + d) % 4, k)))

    def rows_pass(q):
        for d in range(1, 4):
            other = (z + d) % 4
            arrived(yr.at[q, k, other], za_recv.at[q, other])
        half = yr.at[q, k]
        send(copy_to(half, half, e_send.at[q], e_recv.at[q], dev(x, y, z, 1 - k)))

    def rows_finish(q):
        arrived(yr.at[q, 1 - k], e_recv.at[q])

    def column_start(q):
        for d in range(1, 8):
            other = (col + d) % 8
            send(copy_to(sb.at[q, other], cb.at[q, col], gc_send.at[q, d - 1], gc_recv.at[q, col],
                         (row, other)))
        cb[q, col] = sb[q, col]

    def column_finish(q):
        for d in range(1, 8):
            other = (col + d) % 8
            arrived(cb.at[q, other], gc_recv.at[q, other])
        total = cb[q, 0]
        for n in range(1, 8):
            total = total + cb[q, n]
        xb[1, x, :, q * 128:(q + 1) * 128] = total

    def sum_start(g):
        for d in range(1, 4):
            send(copy_to(xb.at[g, x], xb.at[g, x], gx_send.at[g, d - 1], gx_recv.at[g, x],
                         dev((x + d) % 4, y, z, k)))

    def sum_middle(g):
        for d in range(1, 4):
            other = (x + d) % 4
            arrived(xb.at[g, other], gx_recv.at[g, other])
        yb[g, y] = xb[g, 0] + xb[g, 1] + xb[g, 2] + xb[g, 3]
        for d in range(1, 4):
            send(copy_to(yb.at[g, y], yb.at[g, y], gy_send.at[g, d - 1], gy_recv.at[g, y],
                         dev(x, (y + d) % 4, z, k)))

    def sum_gather(g):
        for d in range(1, 4):
            other = (y + d) % 4
            arrived(yb.at[g, other], gy_recv.at[g, other])
        gb[g, col] = yb[g, 0] + yb[g, 1] + yb[g, 2] + yb[g, 3]
        for d in range(1, 8):
            send(copy_to(gb.at[g, col], gb.at[g, col], gg_send.at[g, d - 1], gg_recv.at[g, col],
                         (row, (col + d) % 8)))

    def sum_finish(g):
        for d in range(1, 8):
            other = (col + d) % 8
            arrived(gb.at[g, other], gg_recv.at[g, other])

    def own_rows(ref, m):
        here = (m // 2, pl.ds(2 * (m % 2), 2))
        return jnp.concatenate(
            [ref[(0,) + here].reshape(256, 128), ref[(1,) + here].reshape(256, 128)], axis=1
        )

    def inner(target, right_of):
        def part(m, carry):
            left_part = vt[:, pl.ds(pl.multiple_of(m * 256, 256), 256)]
            piece = exact(left_part, right_of(m), NN).reshape(target.shape)

            @pl.when(m == 0)
            def _():
                target[...] = piece

            @pl.when(m > 0)
            def _():
                target[...] = target[...] + piece

            return carry

        lax.fori_loop(0, 4, part, 0)

    def product_rows(q):
        return lambda m: yp[q, m // 2, pl.ds(2 * (m % 2), 2)].reshape(256, 128)

    ri = lax.broadcasted_iota(jnp.int32, (256, 256), 0)
    ci = lax.broadcasted_iota(jnp.int32, (256, 256), 1)

    def eye():
        return jnp.where(ri == ci, 1.0, 0.0).astype(F32)

    def factor_start():
        gram = gb[0].reshape(256, 256)
        halves = jnp.sum(jnp.where(ri == ci, gram, 0.0), axis=0, keepdims=True) * 0.5
        block = jnp.logical_and(ri // 64 == ci // 64, ci > ri)
        negated = -(jnp.where(block, gram, 0.0) / halves)
        pw[...] = negated
        inv[...] = eye() + negated

    def factor_double(step, carry):
        power = exact(pw[...], pw[...], NN)
        pw[...] = power
        inv[...] = exact(inv[...], eye() + power, NN)
        return carry

    def factor_scale():
        gram = gb[0].reshape(256, 256)
        halves = jnp.sum(jnp.where(ri == ci, gram, 0.0), axis=1, keepdims=True) * 0.5
        inv[...] = inv[...] / halves

    def factor_join(width):
        gram = gb[0].reshape(256, 256)
        above = jnp.logical_and(ri // (2 * width) == ci // (2 * width), ri // width < ci // width)
        off = jnp.where(above, gram, 0.0)
        inv[...] = inv[...] - exact(exact(inv[...], off, NN), inv[...], NN)

    def place(t):
        b, n = (b_own + t // 4) % 2, t % 4
        h = (n + 1) // 2 % 2
        jp = h * (n - 1) + (1 - h) * ((y // 2 + n // 3) % 2)
        return b, h, jp

    def pair(ref, here):
        return jnp.concatenate(
            [ref[(0,) + here].reshape(256, 128), ref[(1,) + here].reshape(256, 128)], axis=1
        )

    def subtract(i, high_ref, low_ref, right, store):
        high, low = split(right)
        right = jnp.concatenate([high, low, high], axis=1)

        left_high = high_ref[...]
        left = jnp.concatenate([left_high, left_high, low_ref[...]], axis=1)
        store(a_buf[i] - quick(left, right, NT))

    def begin(i, carry):
        here = (i // 4, i // 2 % 2, pl.ds(2 * (i % 2), 2))

        def store(value):
            a_buf[i] = value

        subtract(i, lhi_ref, llo_ref, pair(vc, here), store)
        return carry

    def finish(t, carry):
        b, h, jp = place(t)
        for q in range(2):
            for n in range(2):
                step_d(1, q, b, h, 2 * jp + n)
        here = (b, h, pl.ds(2 * jp, 2))
        i = b * 4 + h * 2 + jp
        high, low = split(jnp.concatenate([pair(yc, here), pair(vc, here)], axis=1))
        total = quick(jnp.concatenate([high, high, low], axis=1), tm[...], NN)
        columns = pl.ds(pl.multiple_of(i * 256, 256), 256)

        def store(value):
            out_ref[:, columns] = value

        subtract(i, vhi_ref, vlo_ref, total, store)
        return carry

    panel_start(0)
    panel_start(1)
    inner(pb, lambda m: own_rows(vr, m))
    xb[0, x] = pb[col]
    sum_start(0)
    step_a(0, 0)
    sum_middle(0)

    for i in range(8):
        slab(i).wait()

        def chop(m, carry):
            rows = pl.ds(pl.multiple_of(m * 128, 128), 128)
            high, low = split(a_buf[i, rows])
            a_hi[i, rows] = high
            a_lo[i, rows] = low
            return carry

        lax.fori_loop(0, 8, chop, 0)
        if i == 3:
            step_b(0, 0)
            step_c(0, 0)
    step_a(0, 1)
    multiply(0, 0)
    multiply(0, 1)
    step_b(0, 1)
    step_c(0, 1)
    multiply(0, 2)
    multiply(0, 3)
    pair_start(0)
    sum_gather(0)
    inner(sb.at[0], product_rows(0))
    scatter_start(0)
    column_start(0)
    multiply(1, 0)
    multiply(1, 1)
    scatter_finish(0)
    multiply(1, 2)
    multiply(1, 3)
    pair_start(1)
    inner(sb.at[1], product_rows(1))
    scatter_start(1)
    column_start(1)
    step_a(1, 0)
    sum_finish(0)
    factor_start()
    column_finish(0)
    scatter_finish(1)
    column_finish(1)
    sum_start(1)
    step_b(1, 0)
    rows_pass(0)
    lax.fori_loop(0, 5, factor_double, 0)
    factor_scale()
    factor_join(64)
    factor_join(128)
    step_a(1, 1)

    def split_rows(m, carry):
        rows = pl.ds(pl.multiple_of(m * 256, 256), 256)
        high, low = split(own_rows(vr, m))
        vhi_ref[rows] = high
        vlo_ref[rows] = low
        return carry

    sum_middle(1)
    step_c(1, 0)
    rows_pass(1)
    rows_finish(0)
    lax.fori_loop(0, 4, split_rows, 0)
    step_b(1, 1)
    step_c(1, 1)
    sum_gather(1)
    rows_finish(1)

    def left_update(m, carry):
        rows = pl.ds(pl.multiple_of(m * 256, 256), 256)
        high, low = split(exact(own_rows(yr, m), inv[...], NN))
        lhi_ref[rows] = high
        llo_ref[rows] = low
        return carry

    lax.fori_loop(0, 4, left_update, 0)
    lax.fori_loop(0, 8, begin, 0)
    sum_finish(1)
    inner_factor = inv[...]
    coupling = exact(inner_factor.T, exact(gb[1].reshape(256, 256), inner_factor, NN), NN)
    high, low = split(inner_factor)
    tm[0:256] = high
    tm[512:768] = low
    tm[1024:1280] = high
    high, low = split(-coupling)
    tm[256:512] = high
    tm[768:1024] = low
    tm[1280:1536] = high
    lax.fori_loop(0, 8, finish, 0)

    for copy, cond in sent:
        if cond is None:
            copy.wait_send()
        else:
            pl.when(cond)(copy.wait_send)


def exchange(trailing, raw):
    dma = pltpu.SemaphoreType.DMA
    pieces = pltpu.VMEM((2, 2, 2, 4, 128, 128), F32)
    by_rows = pltpu.VMEM((2, 2, 4, 128, 128), F32)
    halves = pltpu.VMEM((2, 4, 128, 128), F32)
    whole = pltpu.VMEM((2, 8, 32, 256), F32)
    slices = pltpu.VMEM((2, 4, 32, 256), F32)
    square = pltpu.VMEM((256, 256), F32)
    left = pltpu.VMEM((1024, 256), BF16)
    columns = pltpu.VMEM((2, 8, 32, 128), F32)
    return pl.pallas_call(
        exchange_kernel,
        out_shape=jax.ShapeDtypeStruct(trailing.shape, F32),
        in_specs=[
            pl.BlockSpec(memory_space=pl.ANY),
            pl.BlockSpec(memory_space=pltpu.VMEM),
        ],
        out_specs=pl.BlockSpec(memory_space=pltpu.VMEM),
        scratch_shapes=[
            pltpu.VMEM((8, 1024, 256), F32),
            pltpu.VMEM((8, 1024, 256), BF16),
            pltpu.VMEM((8, 1024, 256), BF16),
            pltpu.VMEM((256, 1024), F32),
            by_rows, pieces, pieces, by_rows, halves, halves, halves,
            pltpu.VMEM((2, 128, 128), F32),
            by_rows, pltpu.VMEM((8, 32, 256), F32), columns, columns, slices, slices, whole,
            square, square, pltpu.VMEM((1536, 256), BF16), left, left, left, left,
            dma((8,)),
            dma((2, 2, 4)),
            dma((2, 2, 2)),
            dma((2, 2, 9, 3)),
            dma((2, 2, 2, 2, 4)),
            dma((2,)),
            dma((2,)),
            dma((2, 3)),
            dma((2, 4)),
            dma((2, 3)),
            dma((2, 4)),
            dma((2,)),
            dma((2,)),
            dma((2, 7)),
            dma((2, 8)),
            dma((2, 3)),
            dma((2, 4)),
            dma((2, 3)),
            dma((2, 4)),
            dma((2, 7)),
            dma((2, 8)),
        ],
        compiler_params=pltpu.CompilerParams(
            collective_id=0, has_side_effects=True, vmem_limit_bytes=44 * 1024 * 1024
        ),
        cost_estimate=pl.CostEstimate(
            flops=8_000_000_000, bytes_accessed=16 * 1024 * 1024, transcendentals=0
        ),
        name="exchange",
    )(trailing, raw)


def local(trailing, reflectors):
    raw = jnp.swapaxes(reflectors, 1, 2).reshape(256, 1024)
    return exchange(trailing, raw)


def solution(mesh):
    placed = (P("row", "col"), P(None, "row", None))
    return jax.shard_map(
        local, mesh=mesh, in_specs=placed, out_specs=P("row", "col"), check_vma=False
    )
```

```python
import jax
import jax.numpy as jnp
from jax import lax
from jax.experimental import pallas as pl
from jax.experimental.pallas import tpu as pltpu
from jax.sharding import PartitionSpec as P

MESH = pl.DeviceIdType.MESH
F32 = jnp.float32
BF16 = jnp.bfloat16


def exact(left, right, dims):
    return lax.dot_general(
        left, right, (dims, ((), ())), precision=lax.Precision.HIGHEST, preferred_element_type=F32
    )


def quick(left, right, dims):
    return lax.dot_general(left, right, (dims, ((), ())), preferred_element_type=F32)


def split(value):
    high = value.astype(BF16)
    low = (value - high.astype(F32)).astype(BF16)
    return high, low


NN = ((1,), (0,))
NT = ((1,), (1,))


def exchange_kernel(
    a_hbm, raw_ref,
    out_ref,
    a_buf, a_hi, a_lo, vt, vr, vc, yc, yp, drx, yh, zrx, ys, yr,
    pb, sb, cb, xb, yb, gb, pw, inv, tm, lhi_ref, llo_ref, vhi_ref, vlo_ref,
    a_sem,
    t_send, t_recv, p_send, p_recv,
    d_send, d_recv, zr_send, zr_recv, za_send, za_recv, e_send, e_recv,
    gc_send, gc_recv, gx_send, gx_recv, gy_send, gy_recv, gg_send, gg_recv,
):
    row = lax.axis_index("row")
    col = lax.axis_index("col")
    x, y = row % 4, row // 4
    z, k = col // 2, col % 2

    def dev(dx, dy, dz, dk):
        return (dy * 4 + dx, dz * 2 + dk)

    def copy_to(src, dst, send, recv, device):
        return pltpu.make_async_remote_copy(
            src_ref=src, dst_ref=dst, send_sem=send, recv_sem=recv,
            device_id=device, device_id_type=MESH,
        )

    def arrived(dst, recv):
        copy_to(dst, dst, recv, recv, dev(x, y, z, 1 - k)).wait_recv()

    sent = []

    def send(copy, cond=None):
        if cond is None:
            copy.start()
        else:
            pl.when(cond)(copy.start)
        sent.append((copy, cond))

    is_src = k == x // 2
    b_own = x % 2
    stays = jnp.logical_and(y == z, is_src)

    def slab(i):
        return pltpu.make_async_copy(
            a_hbm.at[:, pl.ds(i * 256, 256)], a_buf.at[i], a_sem.at[i]
        )

    for i in range(8):
        slab(i).start()

    barrier = pltpu.get_barrier_semaphore()

    def greet(device):
        pl.semaphore_signal(barrier, inc=1, device_id=device, device_id_type=MESH)

    for d in range(1, 4):
        greet(dev((x + d) % 4, y, z, k))
        greet(dev(x, (y + d) % 4, z, 0))
        greet(dev(x, (y + d) % 4, z, 1))
    for d in range(1, 8):
        greet((row, (col + d) % 8))

    @pl.when(y != z)
    def _():
        greet(dev(x, z, y, 0))
        greet(dev(x, z, y, 1))

    for n in range(8):
        for q in range(2):
            piece = raw_ref[q * 128:(q + 1) * 128, n * 128:(n + 1) * 128]
            here = row * 1024 + n * 128 + lax.broadcasted_iota(jnp.int32, (128, 128), 1)
            pivot = (q * 128 + 64) + lax.broadcasted_iota(jnp.int32, (128, 128), 0)
            ones_part = jnp.where(here == pivot, 1.0, 0.0).astype(F32)
            piece = jnp.where(here > pivot, piece, ones_part)
            vt[q * 128:(q + 1) * 128, n * 128:(n + 1) * 128] = piece
            vr[q, n // 4, n % 4] = piece.T

    pl.semaphore_wait(barrier, jnp.where(y != z, 18, 16))

    def panel_start(q):
        for d in range(4):
            j = (y + d) % 4
            send(
                copy_to(vr.at[q, k, j], vc.at[q, b_own, k, j], t_send.at[0, q, d],
                        t_recv.at[0, q, k], dev(x, j, z, x // 2)),
                y == z if d else jnp.logical_and(y == z, jnp.logical_not(is_src)),
            )

        @pl.when(stays)
        def _():
            vc[q, b_own, k, y] = vr[q, k, y]

    def product_start(q):
        send(
            copy_to(ys.at[q], yc.at[q, b_own, k, z], t_send.at[1, q, 0], t_recv.at[1, q, k],
                    dev(x, z, y, x // 2)),
            jnp.logical_not(stays),
        )

        @pl.when(stays)
        def _():
            yc[q, b_own, k, z] = ys[q]

    def spread(ph, q, slot, b, h, j, along_x, cond):
        piece = (vc if ph == 0 else yc).at[q, b, h, j]
        for d in range(1, 4):
            device = dev((x + d) % 4, y, z, k) if along_x else dev(x, (y + d) % 4, z, k)
            send(
                copy_to(piece, piece, p_send.at[ph, q, slot, d - 1], p_recv.at[ph, q, b, h, j],
                        device),
                cond,
            )

    def piece_in(ph, q, b, h, j, cond):
        @pl.when(cond)
        def _():
            arrived((vc if ph == 0 else yc).at[q, b, h, j], p_recv.at[ph, q, b, h, j])

    def step_a(ph, q):
        target = vc if ph == 0 else yc
        for h in range(2):
            @pl.when(jnp.logical_and(
                is_src, jnp.logical_not(jnp.logical_and(y == z, k == h))))
            def _():
                arrived(target.at[q, b_own, h, y], t_recv.at[ph, q, h])

            spread(ph, q, 2 * h, b_own, h, y, h == 1, is_src)
            spread(ph, q, 2 * h + 1, b_own, h, y, h == 0, is_src)

    def step_b(ph, q):
        for n, delta in enumerate((1, 3, 2)):
            j = (y + 4 - delta) % 4
            piece_in(ph, q, b_own, 0, j, is_src)
            spread(ph, q, 4 + n, b_own, 0, j, True, is_src)

    def foreign(b):
        return jnp.logical_not(jnp.logical_and(is_src, b_own == b))

    def step_c(ph, q):
        for b in range(2):
            piece_in(ph, q, b, 1, y, foreign(b))
            spread(ph, q, 7 + b, b, 1, y, False, foreign(b))

    def step_d(ph, q, b, h, j):
        piece_in(ph, q, b, h, j, jnp.logical_or(
            jnp.logical_and(h == 0, foreign(b)), jnp.logical_and(h == 1, y != j)))

    def multiply(q, t):
        b, h = (b_own + t // 2) % 2, t % 2
        for j in range(4):
            step_d(0, q, b, h, j)
        high, low = split(vc[q, b, h].reshape(512, 128))
        both = jnp.concatenate([high, low], axis=1)
        i = b * 4 + h * 2

        def tile(m, carry):
            rows = pl.ds(pl.multiple_of(m * 512, 512), 512)
            wide = quick(jnp.concatenate([a_hi[i, rows], a_hi[i + 1, rows]], axis=1), both, NN)
            slim = quick(jnp.concatenate([a_lo[i, rows], a_lo[i + 1, rows]], axis=1), high, NN)
            part = (wide[:, :128] + wide[:, 128:] + slim).reshape(4, 128, 128)
            if t == 0:
                yp[q, m] = part
            else:
                yp[q, m] = yp[q, m] + part
            return carry

        lax.fori_loop(0, 2, tile, 0)

    def pair_start(q):
        send(copy_to(yp.at[q, 1 - k], drx.at[q], d_send.at[q], d_recv.at[q],
                     dev(x, y, z, 1 - k)))

    def scatter_start(q):
        arrived(drx.at[q], d_recv.at[q])
        yh[q] = yp[q, k] + drx[q]
        for d in range(1, 4):
            other = (z + d) % 4
            send(copy_to(yh.at[q, other], zrx.at[q, z], zr_send.at[q, d - 1], zr_recv.at[q, z],
                         dev(x, y, other, k)))
        zrx[q, z] = yh[q, z]

    def scatter_finish(q):
        for d in range(1, 4):
            other = (z + d) % 4
            arrived(zrx.at[q, other], zr_recv.at[q, other])
        total = zrx[q, 0] + zrx[q, 1] + zrx[q, 2] + zrx[q, 3]
        ys[q] = total
        yr[q, k, z] = total
        product_start(q)
        for d in range(1, 4):
            send(copy_to(ys.at[q], yr.at[q, k, z], za_send.at[q, d - 1], za_recv.at[q, z],
                         dev(x, y, (z + d) % 4, k)))

    def rows_pass(q):
        for d in range(1, 4):
            other = (z + d) % 4
            arrived(yr.at[q, k, other], za_recv.at[q, other])
        half = yr.at[q, k]
        send(copy_to(half, half, e_send.at[q], e_recv.at[q], dev(x, y, z, 1 - k)))

    def rows_finish(q):
        arrived(yr.at[q, 1 - k], e_recv.at[q])

    def column_start(q):
        for d in range(1, 8):
            other = (col + d) % 8
            send(copy_to(sb.at[q, other], cb.at[q, col], gc_send.at[q, d - 1], gc_recv.at[q, col],
                         (row, other)))
        cb[q, col] = sb[q, col]

    def column_finish(q):
        for d in range(1, 8):
            other = (col + d) % 8
            arrived(cb.at[q, other], gc_recv.at[q, other])
        total = cb[q, 0]
        for n in range(1, 8):
            total = total + cb[q, n]
        xb[1, x, :, q * 128:(q + 1) * 128] = total

    def sum_start(g):
        for d in range(1, 4):
            send(copy_to(xb.at[g, x], xb.at[g, x], gx_send.at[g, d - 1], gx_recv.at[g, x],
                         dev((x + d) % 4, y, z, k)))

    def sum_middle(g):
        for d in range(1, 4):
            other = (x + d) % 4
            arrived(xb.at[g, other], gx_recv.at[g, other])
        yb[g, y] = xb[g, 0] + xb[g, 1] + xb[g, 2] + xb[g, 3]
        for d in range(1, 4):
            send(copy_to(yb.at[g, y], yb.at[g, y], gy_send.at[g, d - 1], gy_recv.at[g, y],
                         dev(x, (y + d) % 4, z, k)))

    def sum_gather(g):
        for d in range(1, 4):
            other = (y + d) % 4
            arrived(yb.at[g, other], gy_recv.at[g, other])
        gb[g, col] = yb[g, 0] + yb[g, 1] + yb[g, 2] + yb[g, 3]
        for d in range(1, 8):
            send(copy_to(gb.at[g, col], gb.at[g, col], gg_send.at[g, d - 1], gg_recv.at[g, col],
                         (row, (col + d) % 8)))

    def sum_finish(g):
        for d in range(1, 8):
            other = (col + d) % 8
            arrived(gb.at[g, other], gg_recv.at[g, other])

    def own_rows(ref, m):
        here = (m // 2, pl.ds(2 * (m % 2), 2))
        return jnp.concatenate(
            [ref[(0,) + here].reshape(256, 128), ref[(1,) + here].reshape(256, 128)], axis=1
        )

    def inner(target, right_of):
        def part(m, carry):
            left_part = vt[:, pl.ds(pl.multiple_of(m * 256, 256), 256)]
            piece = exact(left_part, right_of(m), NN).reshape(target.shape)

            @pl.when(m == 0)
            def _():
                target[...] = piece

            @pl.when(m > 0)
            def _():
                target[...] = target[...] + piece

            return carry

        lax.fori_loop(0, 4, part, 0)

    def product_rows(q):
        return lambda m: yp[q, m // 2, pl.ds(2 * (m % 2), 2)].reshape(256, 128)

    ri = lax.broadcasted_iota(jnp.int32, (256, 256), 0)
    ci = lax.broadcasted_iota(jnp.int32, (256, 256), 1)

    def eye():
        return jnp.where(ri == ci, 1.0, 0.0).astype(F32)

    def factor_start():
        gram = gb[0].reshape(256, 256)
        halves = jnp.sum(jnp.where(ri == ci, gram, 0.0), axis=0, keepdims=True) * 0.5
        block = jnp.logical_and(ri // 64 == ci // 64, ci > ri)
        negated = -(jnp.where(block, gram, 0.0) / halves)
        pw[...] = negated
        inv[...] = eye() + negated

    def factor_double(step, carry):
        power = exact(pw[...], pw[...], NN)
        pw[...] = power
        inv[...] = exact(inv[...], eye() + power, NN)
        return carry

    def factor_scale():
        gram = gb[0].reshape(256, 256)
        halves = jnp.sum(jnp.where(ri == ci, gram, 0.0), axis=1, keepdims=True) * 0.5
        inv[...] = inv[...] / halves

    def factor_join(width):
        gram = gb[0].reshape(256, 256)
        above = jnp.logical_and(ri // (2 * width) == ci // (2 * width), ri // width < ci // width)
        off = jnp.where(above, gram, 0.0)
        inv[...] = inv[...] - exact(exact(inv[...], off, NN), inv[...], NN)

    def place(t):
        b, n = (b_own + t // 4) % 2, t % 4
        h = (n + 1) // 2 % 2
        jp = h * (n - 1) + (1 - h) * ((y // 2 + n // 3) % 2)
        return b, h, jp

    def pair(ref, here):
        return jnp.concatenate(
            [ref[(0,) + here].reshape(256, 128), ref[(1,) + here].reshape(256, 128)], axis=1
        )

    def subtract(i, high_ref, low_ref, right, store):
        high, low = split(right)
        right = jnp.concatenate([high, low, high], axis=1)

        left_high = high_ref[...]
        left = jnp.concatenate([left_high, left_high, low_ref[...]], axis=1)
        store(a_buf[i] - quick(left, right, NT))

    def begin(i, carry):
        here = (i // 4, i // 2 % 2, pl.ds(2 * (i % 2), 2))

        def store(value):
            a_buf[i] = value

        subtract(i, lhi_ref, llo_ref, pair(vc, here), store)
        return carry

    def finish(t, carry):
        b, h, jp = place(t)
        for q in range(2):
            for n in range(2):
                step_d(1, q, b, h, 2 * jp + n)
        here = (b, h, pl.ds(2 * jp, 2))
        i = b * 4 + h * 2 + jp
        high, low = split(jnp.concatenate([pair(yc, here), pair(vc, here)], axis=1))
        total = quick(jnp.concatenate([high, high, low], axis=1), tm[...], NN)
        columns = pl.ds(pl.multiple_of(i * 256, 256), 256)

        def store(value):
            out_ref[:, columns] = value

        subtract(i, vhi_ref, vlo_ref, total, store)
        return carry

    panel_start(0)
    panel_start(1)
    inner(pb, lambda m: own_rows(vr, m))
    xb[0, x] = pb[col]
    sum_start(0)
    step_a(0, 0)
    sum_middle(0)

    for i in range(8):
        slab(i).wait()

        def chop(m, carry):
            rows = pl.ds(pl.multiple_of(m * 128, 128), 128)
            high, low = split(a_buf[i, rows])
            a_hi[i, rows] = high
            a_lo[i, rows] = low
            return carry

        lax.fori_loop(0, 8, chop, 0)
        if i == 3:
            step_b(0, 0)
            step_c(0, 0)
    step_a(0, 1)
    multiply(0, 0)
    multiply(0, 1)
    step_b(0, 1)
    step_c(0, 1)
    multiply(0, 2)
    multiply(0, 3)
    pair_start(0)
    sum_gather(0)
    inner(sb.at[0], product_rows(0))
    scatter_start(0)
    column_start(0)
    multiply(1, 0)
    multiply(1, 1)
    scatter_finish(0)
    multiply(1, 2)
    multiply(1, 3)
    pair_start(1)
    inner(sb.at[1], product_rows(1))
    column_start(1)
    scatter_start(1)
    step_a(1, 0)
    sum_finish(0)
    factor_start()
    column_finish(0)
    column_finish(1)
    sum_start(1)
    scatter_finish(1)
    step_b(1, 0)
    rows_pass(0)
    lax.fori_loop(0, 5, factor_double, 0)

    def split_rows(m, carry):
        rows = pl.ds(pl.multiple_of(m * 256, 256), 256)
        high, low = split(own_rows(vr, m))
        vhi_ref[rows] = high
        vlo_ref[rows] = low
        return carry

    sum_middle(1)
    step_a(1, 1)
    step_c(1, 0)
    rows_pass(1)
    rows_finish(0)
    lax.fori_loop(0, 4, split_rows, 0)
    factor_scale()
    factor_join(64)
    factor_join(128)
    sum_gather(1)
    step_b(1, 1)
    step_c(1, 1)
    rows_finish(1)

    def left_update(m, carry):
        rows = pl.ds(pl.multiple_of(m * 256, 256), 256)
        high, low = split(exact(own_rows(yr, m), inv[...], NN))
        lhi_ref[rows] = high
        llo_ref[rows] = low
        return carry

    lax.fori_loop(0, 4, left_update, 0)
    lax.fori_loop(0, 8, begin, 0)
    sum_finish(1)
    inner_factor = inv[...]
    coupling = exact(inner_factor.T, exact(gb[1].reshape(256, 256), inner_factor, NN), NN)
    high, low = split(inner_factor)
    tm[0:256] = high
    tm[512:768] = low
    tm[1024:1280] = high
    high, low = split(-coupling)
    tm[256:512] = high
    tm[768:1024] = low
    tm[1280:1536] = high
    lax.fori_loop(0, 8, finish, 0)

    for copy, cond in sent:
        if cond is None:
            copy.wait_send()
        else:
            pl.when(cond)(copy.wait_send)


def exchange(trailing, raw):
    dma = pltpu.SemaphoreType.DMA
    pieces = pltpu.VMEM((2, 2, 2, 4, 128, 128), F32)
    by_rows = pltpu.VMEM((2, 2, 4, 128, 128), F32)
    halves = pltpu.VMEM((2, 4, 128, 128), F32)
    whole = pltpu.VMEM((2, 8, 32, 256), F32)
    slices = pltpu.VMEM((2, 4, 32, 256), F32)
    square = pltpu.VMEM((256, 256), F32)
    left = pltpu.VMEM((1024, 256), BF16)
    columns = pltpu.VMEM((2, 8, 32, 128), F32)
    return pl.pallas_call(
        exchange_kernel,
        out_shape=jax.ShapeDtypeStruct(trailing.shape, F32),
        in_specs=[
            pl.BlockSpec(memory_space=pl.ANY),
            pl.BlockSpec(memory_space=pltpu.VMEM),
        ],
        out_specs=pl.BlockSpec(memory_space=pltpu.VMEM),
        scratch_shapes=[
            pltpu.VMEM((8, 1024, 256), F32),
            pltpu.VMEM((8, 1024, 256), BF16),
            pltpu.VMEM((8, 1024, 256), BF16),
            pltpu.VMEM((256, 1024), F32),
            by_rows, pieces, pieces, by_rows, halves, halves, halves,
            pltpu.VMEM((2, 128, 128), F32),
            by_rows, pltpu.VMEM((8, 32, 256), F32), columns, columns, slices, slices, whole,
            square, square, pltpu.VMEM((1536, 256), BF16), left, left, left, left,
            dma((8,)),
            dma((2, 2, 4)),
            dma((2, 2, 2)),
            dma((2, 2, 9, 3)),
            dma((2, 2, 2, 2, 4)),
            dma((2,)),
            dma((2,)),
            dma((2, 3)),
            dma((2, 4)),
            dma((2, 3)),
            dma((2, 4)),
            dma((2,)),
            dma((2,)),
            dma((2, 7)),
            dma((2, 8)),
            dma((2, 3)),
            dma((2, 4)),
            dma((2, 3)),
            dma((2, 4)),
            dma((2, 7)),
            dma((2, 8)),
        ],
        compiler_params=pltpu.CompilerParams(
            collective_id=0, has_side_effects=True, vmem_limit_bytes=44 * 1024 * 1024
        ),
        cost_estimate=pl.CostEstimate(
            flops=8_000_000_000, bytes_accessed=16 * 1024 * 1024, transcendentals=0
        ),
        name="exchange",
    )(trailing, raw)


def local(trailing, reflectors):
    raw = jnp.swapaxes(reflectors, 1, 2).reshape(256, 1024)
    return exchange(trailing, raw)


def solution(mesh):
    placed = (P("row", "col"), P(None, "row", None))
    return jax.shard_map(
        local, mesh=mesh, in_specs=placed, out_specs=P("row", "col"), check_vma=False
    )
```
